128 devices in a mesh: node: 32 (over x, z, core), feat: 4 (over y).
Axes of the slice: x: 4, y: 4, z: 4, core: 2. Of those that a mesh axis runs over, the one named last changes fastest.
Arguments:
- features: bfloat16 [100, 32768], P('feat', 'node'), may hold values from -6 to 6
- edges_one: int32 [1024, 32768], P(None, 'node'), may hold values from 0 to 1, as said below
- w1_self: bfloat16 [100, 256], P('feat'), may hold values from -0.625 to 0.625
- w1_nbr: bfloat16 [100, 256], P('feat'), may hold values from -1.25 to 1.25
- need_blocks: int32 [32, 4], P('node'), may hold values from 0 to 31, as said below
- live_slots: int32 [32, 4], P('node'), may hold values from 0 to 1, as said below
- edges_two: int32 [4096, 32768], P(None, 'node'), may hold values from 0 to 1, as said below
- w2_self: bfloat16 [256, 47], P('feat'), may hold values from -0.375 to 0.375
- w2_nbr: bfloat16 [256, 47], P('feat'), may hold values from -0.5 to 0.5
- labels: int32 [32768], P('node'), may hold values from 0 to 46
Outputs:
- node_loss: float32 [32768], P('node')
- mean_loss: float32 [], replicated
The draws below stay inside these ranges and needn't reach their ends.
Inputs may be any that keep to these rules, and one draw needn't show every extreme that they name: `need_blocks`: row b holds 4 different blocks; its first entry is b, its second is b plus half the number of blocks, its third is b minus 1, and its entry k is b plus an offset that depends on k alone, modulo the number of blocks. `live_slots`: the first three entries of each row are 1. `edges_one`: each column has exactly 25 ones. `edges_two`: each column t has exactly 10 ones, all in rows of slots that live_slots marks as used for t's block.
All inputs are finite; a program needn't handle non-finite values.
Results may differ from the reference program's by a relative error of at most 0.00065.
Values may be sent and summed in bfloat16 or wider, within the bound.
No kernel may reach another device: no remote copies, remote signals or barrier semaphores. Data moves between devices by JAX's collectives and lax.ppermute only.
A program may use at most 128 MiB of HBM per device.

```python
import jax
import jax.numpy as jnp
from jax import lax

F = 100
H = 256
C = 47
FAN1 = 25
FAN2 = 10
NEED = 4
BLK = 1024
NODES = 32768


def routing_tables(key):
    blocks = NODES // BLK
    offsets = jnp.arange(blocks, dtype=jnp.int32)
    scores = jax.random.randint(jax.random.fold_in(key, 12), (blocks,), 0, 2 ** 20) * blocks + offsets
    scores = jnp.where(offsets == blocks - 1, 2 ** 30 - 2, scores)
    scores = jnp.where(offsets == blocks // 2, 2 ** 30 - 1, scores)
    scores = jnp.where(offsets == 0, 2 ** 30, scores)
    chosen = lax.top_k(scores, NEED)[1].astype(jnp.int32)
    need = (jnp.arange(blocks, dtype=jnp.int32)[:, None] + chosen[None, :]) % blocks
    level = jax.random.randint(jax.random.fold_in(key, 13), (blocks, 1), 0, NEED + 1)
    coins = jax.random.randint(jax.random.fold_in(key, 14), (blocks, NEED), 0, NEED)
    slots = jnp.arange(NEED, dtype=jnp.int32)[None, :]
    live = jnp.where((slots < 3) | (coins < level), 1, 0).astype(jnp.int32)
    return (need.astype(jnp.int32), live)


def draw_need_blocks(key, part):
    return routing_tables(key)[0]


def draw_live_slots(key, part):
    return routing_tables(key)[1]


def draw_edges_two(key, part):
    need, live = routing_tables(key)
    width = NEED * BLK
    rows = jnp.arange(width, dtype=jnp.int32)[None, :]
    targets = jnp.arange(NODES, dtype=jnp.int32)
    used = live[targets // BLK][:, rows[0] // BLK]
    scores = jax.random.randint(jax.random.fold_in(key, 15), (NODES, width), 0, 2 ** 18) * width + rows
    scores = jnp.where(used == 1, scores, scores - 2 ** 30)
    chosen = lax.top_k(scores, FAN2)[1].astype(jnp.int32)
    return jnp.zeros((width, NODES), jnp.int32).at[chosen, targets[:, None]].set(1)


def draw_edges_one(key, part):
    rows = jnp.arange(BLK, dtype=jnp.int32)[None, :]
    targets = jnp.arange(NODES, dtype=jnp.int32)
    scores = jax.random.randint(jax.random.fold_in(key, 21), (NODES, BLK), 0, 2 ** 18) * BLK + rows
    chosen = lax.top_k(scores, FAN1)[1].astype(jnp.int32)
    return jnp.zeros((BLK, NODES), jnp.int32).at[chosen, targets[:, None]].set(1)


def place_ends(values, rng, least, top_value):
    spot = [jax.random.randint(jax.random.fold_in(rng, axis), (), 0, length) for axis, length in enumerate(values.shape)]
    longest = values.shape.index(max(values.shape))
    next_to = spot[:longest] + [(spot[longest] + 1) % values.shape[longest]] + spot[longest + 1:]
    return values.at[tuple(spot)].set(least).at[tuple(next_to)].set(top_value)


def levels(own_key, extent, shards, least, high):
    def one(axis_at, shards_of):
        heights = jax.random.uniform(jax.random.fold_in(jax.random.fold_in(own_key, 6), axis_at), (shards_of,), jnp.float32, least / len(shards), high / len(shards))
        return jnp.repeat(jnp.exp(heights), extent[axis_at] // shards_of).reshape((-1,) + (1,) * (len(extent) - axis_at - 1))

    level = one(*shards[0])
    for cut in shards[1:]:
        level = level * one(*cut)
    return level


def normal_values(stream_key, dims, deviation, most, split=(), kind=jnp.bfloat16):
    level = levels(stream_key, dims, split, -0.22, 0.18) if split else 1.0
    values = jax.random.normal(stream_key, dims, jnp.float32) * deviation * level
    return jnp.minimum(jnp.maximum(values, -most), most).astype(kind)


def setup_inputs(seed: int = 0) -> dict:
    keys = jax.random.split(jax.random.key(seed), 11)
    features = normal_values(keys[0], (F, NODES), 1.0, 6.0, ((0, 4), (1, 32)))
    edges_one = draw_edges_one(jax.random.fold_in(keys[10], 71), 0)
    w1_self = normal_values(keys[2], (F, H), F ** -0.5, 0.625, ((0, 4),))
    w1_nbr = normal_values(keys[3], (F, H), (F // 4) ** -0.5, 1.25, ((0, 4),))
    need_blocks = draw_need_blocks(jax.random.fold_in(keys[10], 71), 0)
    live_slots = draw_live_slots(jax.random.fold_in(keys[10], 71), 0)
    edges_two = draw_edges_two(jax.random.fold_in(keys[10], 71), 0)
    w2_self = normal_values(keys[7], (H, C), H ** -0.5, 0.375, ((0, 4),))
    w2_nbr = normal_values(keys[8], (H, C), (H // 2) ** -0.5, 0.5, ((0, 4),))
    labels = place_ends(jax.random.randint(keys[9], (NODES,), 0, C), jax.random.fold_in(keys[9], 1), 0, C - 1).astype(jnp.int32)
    return {"features": features, "edges_one": edges_one, "w1_self": w1_self, "w1_nbr": w1_nbr, "need_blocks": need_blocks, "live_slots": live_slots, "edges_two": edges_two, "w2_self": w2_self, "w2_nbr": w2_nbr, "labels": labels}


def reference(features, edges_one, w1_self, w1_nbr, need_blocks, live_slots, edges_two, w2_self, w2_nbr, labels):
    blocks = NODES // BLK
    inputs = features.reshape(F, blocks, BLK).transpose(1, 0, 2)
    firsts = edges_one.reshape(BLK, blocks, BLK).transpose(1, 0, 2)

    def first_layer(pair):
        block_x, adjacency = pair
        neighbour = (jnp.dot(block_x, adjacency.astype(jnp.bfloat16), preferred_element_type=jnp.float32) / FAN1).astype(jnp.bfloat16)
        before = jnp.dot(w1_self.T, block_x, preferred_element_type=jnp.float32)
        before = before + jnp.dot(w1_nbr.T, neighbour, preferred_element_type=jnp.float32)
        return jax.nn.relu(before).astype(jnp.bfloat16)

    hidden = lax.map(first_layer, (inputs, firsts))

    def second_layer(block):
        columns = lax.dynamic_slice_in_dim(edges_two, block * BLK, BLK, 1).reshape(NEED, BLK, BLK).astype(jnp.float32)
        weights = live_slots[block].astype(jnp.float32)
        sources = hidden[need_blocks[block]].astype(jnp.float32) * weights[:, None, None]
        gathered = jnp.einsum("khs,kst->ht", sources, columns, precision=lax.Precision.HIGHEST)
        logits = jnp.dot(w2_self.T, hidden[block], preferred_element_type=jnp.float32)
        logits = logits + jnp.dot(w2_nbr.T.astype(jnp.float32), gathered, precision=lax.Precision.HIGHEST) / FAN2
        block_labels = lax.dynamic_slice_in_dim(labels, block * BLK, BLK)
        class_ids = jnp.arange(C, dtype=jnp.int32)[:, None]
        picked = jnp.sum(jnp.where(class_ids == block_labels[None, :], logits, 0.0), 0)
        return jnp.log(jnp.sum(jnp.exp(logits), 0)) - picked

    node_loss = lax.map(second_layer, jnp.arange(blocks, dtype=jnp.int32)).reshape(NODES)
    mean_loss = jnp.sum(node_loss) / NODES
    return node_loss, mean_loss
```

```python
import jax
import jax.numpy as jnp
from jax import lax
from jax.sharding import PartitionSpec as P

FAN1 = 25
FAN2 = 10


def from_ahead(value, axis, steps):
    count = lax.axis_size(axis)
    pairs = [(source, (source - steps) % count) for source in range(count)]
    return lax.ppermute(value, axis, pairs)


def from_everyone(value, axis):
    devices = lax.axis_size(axis)
    return lax.all_to_all(
        jnp.broadcast_to(value[None], (devices, *value.shape)), axis, 0, 0, tiled=True
    )


def all_parts(value, axis):
    devices = lax.axis_size(axis)
    blocks = [value] + [from_ahead(value, axis, step) for step in range(1, devices)]
    order = (jnp.arange(devices) - lax.axis_index(axis)) % devices
    return jnp.take(jnp.stack(blocks, 0), order, axis=0)


def contract(weight, values):
    return lax.dot_general(
        weight, values, (((0,), (0,)), ((), ())), preferred_element_type=jnp.float32
    )


def local(
    features,
    edges_one,
    w1_self,
    w1_nbr,
    need_blocks,
    live_slots,
    edges_two,
    w2_self,
    w2_nbr,
    labels,
):
    block_len = features.shape[1]
    hidden_units = w1_self.shape[1]
    classes = w2_self.shape[1]
    nodes = lax.axis_size("node")
    feats = lax.axis_size("feat")
    mine = lax.axis_index("node")

    w2 = jnp.concatenate([w2_self.T, w2_nbr.T], axis=0)
    packed = jnp.concatenate([features, w1_self, w1_nbr], axis=1)
    parts = all_parts(packed, "feat")
    w2_parts = all_parts(w2, "feat")
    gathered = parts.reshape(-1, packed.shape[1])
    inputs = gathered[:, :block_len]
    w1s = gathered[:, block_len : block_len + hidden_units]
    w1n = gathered[:, block_len + hidden_units :]

    adjacency = edges_one.astype(jnp.bfloat16)
    neighbour = (jnp.dot(inputs, adjacency, preferred_element_type=jnp.float32) / FAN1).astype(
        jnp.bfloat16
    )
    before = contract(w1s, inputs) + contract(w1n, neighbour)
    hidden = jax.nn.relu(before).astype(jnp.bfloat16)

    w2_all = jnp.moveaxis(w2_parts, 0, 1).reshape(2 * classes, hidden_units)
    both = jnp.dot(w2_all, hidden, preferred_element_type=jnp.float32)
    self_term = both[:classes]
    mine_nbr = both[classes:].astype(jnp.bfloat16)

    need_row = need_blocks[0]
    live_row = live_slots[0]
    offset = (need_row[3] - mine) % nodes
    half = from_ahead(mine_nbr, "node", nodes // 2)
    behind = from_ahead(mine_nbr, "node", nodes - 1)
    fourth = lax.switch(
        offset,
        [(lambda value, step=step: from_ahead(value, "node", step)) for step in range(nodes)],
        mine_nbr,
    )
    total = jnp.zeros((classes, block_len), jnp.float32)
    for slot, values in enumerate((mine_nbr, half, behind, fourth)):
        rows = edges_two[slot * block_len : (slot + 1) * block_len].astype(jnp.bfloat16)
        term = jnp.dot(values, rows, preferred_element_type=jnp.float32)
        total = total + jnp.where(live_row[slot] == 1, term, 0.0)
    logits = self_term + total / FAN2
    class_ids = jnp.arange(classes, dtype=jnp.int32)[:, None]
    picked = jnp.sum(jnp.where(class_ids == labels[None, :], logits, 0.0), 0)
    node_loss = jnp.log(jnp.sum(jnp.exp(logits), 0)) - picked
    summed = jnp.sum(from_everyone(jnp.sum(node_loss), "node"))
    mean_loss = summed / (block_len * nodes)
    return (node_loss, mean_loss)


def solution(mesh):
    return jax.shard_map(
        local,
        mesh=mesh,
        in_specs=(
            P("feat", "node"),
            P(None, "node"),
            P("feat", None),
            P("feat", None),
            P("node", None),
            P("node", None),
            P(None, "node"),
            P("feat", None),
            P("feat", None),
            P("node"),
        ),
        out_specs=(P("node"), P()),
        check_vma=False,
    )
```

```python
import functools

import jax
import jax.numpy as jnp
from jax import lax
from jax.experimental import pallas as pl
from jax.experimental.pallas import tpu as pltpu
from jax.sharding import PartitionSpec as P

FAN1 = 25
FAN2 = 10
LANES = 128
MIB = 1 << 20

VMEM = pl.BlockSpec(memory_space=pltpu.VMEM)
HBM = pl.BlockSpec(memory_space=pltpu.HBM)
SMEM = pl.BlockSpec(memory_space=pltpu.SMEM)


def in_hbm(value):
    return pltpu.with_memory_space_constraint(value, pltpu.HBM)


def from_ahead(value, axis, steps):
    count = lax.axis_size(axis)
    pairs = [(source, (source - steps) % count) for source in range(count)]
    return lax.ppermute(value, axis, pairs)


def pack_kernel(nodes, *refs):
    sources, (out_ref, off_ref), held, (scr, cat, sems) = refs[:6], refs[6:8], refs[8:14], refs[14:]
    copies = [
        pltpu.make_async_copy(source, place, sems.at[index])
        for index, (source, place) in enumerate(zip(sources, held))
    ]
    for copy in copies:
        copy.start()
    x_ref, ws_ref, wn_ref, us_ref, un_ref, need_ref = held
    rows, cols = x_ref.shape
    hid = ws_ref.shape[1]
    classes, depth = us_ref.shape
    spare = out_ref.shape[0] - rows
    bands = pl.cdiv(classes, spare)
    scr[rows:, :] = jnp.zeros((spare, scr.shape[1]), jnp.float32)
    for copy in copies:
        copy.wait()
    scr[:rows, :cols] = x_ref[...].astype(jnp.float32)
    scr[:rows, cols : cols + hid] = ws_ref[...].astype(jnp.float32)
    scr[:rows, cols + hid :] = wn_ref[...].astype(jnp.float32)
    cat[:classes, :depth] = us_ref[...].astype(jnp.float32)
    cat[:classes, depth:] = un_ref[...].astype(jnp.float32)
    for band in range(bands):
        first = band * spare
        count = min(spare, classes - first)
        scr[rows : rows + count, band * LANES : (band + 1) * LANES] = cat[first : first + count, :]
    out_ref[...] = scr[...].astype(jnp.bfloat16)
    offset = lax.rem(need_ref[0, 3] - lax.axis_index("node") + nodes, nodes)
    off_ref[0] = offset - 1 - (offset > nodes // 2).astype(jnp.int32)


def load_kernel(splits, e1_ref, e2_ref, after_ref, e1_out, e2_out, sems):
    copies = [pltpu.make_async_copy(e1_ref, e1_out, sems.at[0])]
    rows = e2_out.shape[0] // splits
    for index in range(splits):
        part = pl.ds(index * rows, rows)
        copies.append(pltpu.make_async_copy(e2_ref.at[part], e2_out.at[part], sems.at[index + 1]))
    for copy in copies:
        copy.start()
    for copy in copies:
        copy.wait()


def first_kernel(
    rows, hid, classes, p0_ref, p1_ref, p2_ref, p3_ref, e_ref, self_ref, z_ref, blocks, w2, w1
):
    me = lax.axis_index("feat")
    feats, height, width = blocks.shape
    cols = width - 2 * hid
    spare = height - rows
    for step, ref in enumerate((p0_ref, p1_ref, p2_ref, p3_ref)):
        blocks[lax.rem(me + step, feats)] = ref[...]
    bands = pl.cdiv(classes, spare)
    for f in range(feats):
        for band in range(bands):
            count = min(spare, classes - band * spare)
            tail = blocks[f, :, band * LANES : (band + 1) * LANES].astype(jnp.float32)
            w2[f, band * spare : band * spare + count, :] = tail[rows : rows + count]
        w2[f, classes:, :] = jnp.zeros((w2.shape[1] - classes, LANES), jnp.float32)
    half = LANES // 2
    low = lax.broadcasted_iota(jnp.int32, (w2.shape[1], LANES), 1) < half
    selfs, nbrs = [], []
    for f in range(0, feats, 2):
        a, b = w2[f], w2[f + 1]
        selfs.append(jnp.where(low, a, pltpu.roll(b, half, 1)))
        nbrs.append(jnp.where(low, pltpu.roll(a, half, 1), b))
    project = jnp.concatenate(
        [jnp.concatenate(selfs, axis=1), jnp.concatenate(nbrs, axis=1)], axis=0
    ).astype(jnp.bfloat16)
    inputs = blocks[:, :, :cols].reshape(feats * height, cols)
    w1[: feats * height, :] = blocks[:, :, cols : cols + hid].reshape(feats * height, hid)
    w1[feats * height :, :] = blocks[:, :, cols + hid :].reshape(feats * height, hid)
    weights = w1[...]
    padded = w2.shape[1]
    chunk = 256
    for first in range(0, cols, chunk):
        part = slice(first, first + chunk)
        adjacency = e_ref[:, part].astype(jnp.float32).astype(jnp.bfloat16)
        nbr = jnp.dot(inputs, adjacency, preferred_element_type=jnp.float32) / FAN1
        stacked = jnp.concatenate([inputs[:, part], nbr.astype(jnp.bfloat16)], axis=0)
        before = lax.dot_general(
            weights, stacked, (((0,), (0,)), ((), ())), preferred_element_type=jnp.float32
        )
        hidden = jnp.maximum(before, 0.0).astype(jnp.bfloat16)
        both = jnp.dot(project, hidden, preferred_element_type=jnp.float32)
        self_ref[:, part] = both[:padded]
        z_ref[:, part] = both[padded:].astype(jnp.bfloat16)


def second_kernel(
    classes, z0_ref, z1_ref, z2_ref, z3_ref, self_ref, live_ref, e_ref, label_ref, loss_ref, sum_ref
):
    padded, cols = self_ref.shape
    refs = (z0_ref, z1_ref, z2_ref, z3_ref)
    chunk = 256
    class_ids = lax.broadcasted_iota(jnp.int32, (padded, chunk), 0)

    def step(index, summed):
        part = pl.ds(pl.multiple_of(index * chunk, chunk), chunk)
        total = jnp.zeros((padded, chunk), jnp.float32)
        for slot, ref in enumerate(refs):
            rows = e_ref[slot * cols : (slot + 1) * cols, part]
            rows = rows.astype(jnp.float32).astype(jnp.bfloat16)
            term = jnp.dot(ref[...], rows, preferred_element_type=jnp.float32)
            total = total + jnp.where(live_ref[0, slot] == 1, term, 0.0)
        logits = self_ref[:, part] + total / FAN2
        powers = jnp.where(class_ids < classes, jnp.exp(logits), 0.0)
        picked = jnp.where(class_ids == label_ref[:, part], logits, 0.0)
        loss = jnp.log(jnp.sum(powers, 0, keepdims=True)) - jnp.sum(picked, 0, keepdims=True)
        loss_ref[:, part] = loss
        return summed + jnp.sum(loss, keepdims=True)

    summed = lax.fori_loop(0, cols // chunk, step, jnp.zeros((1, 1), jnp.float32))
    sum_ref[...] = jnp.broadcast_to(summed.reshape(1, 1, 1), sum_ref.shape)


def local(
    features,
    edges_one,
    w1_self,
    w1_nbr,
    need_blocks,
    live_slots,
    edges_two,
    w2_self,
    w2_nbr,
    labels,
):
    rows, block_len = features.shape
    hid = w1_self.shape[1]
    depth, classes = w2_self.shape
    nodes = lax.axis_size("node")
    feats = lax.axis_size("feat")
    height = pl.cdiv(rows, 8) * 8
    width = block_len + 2 * hid
    padded = pl.cdiv(classes, 16) * 16

    packed, number = pl.pallas_call(
        functools.partial(pack_kernel, nodes),
        out_shape=(
            jax.ShapeDtypeStruct((height, width), jnp.bfloat16),
            jax.ShapeDtypeStruct((1,), jnp.int32),
        ),
        in_specs=[HBM] * 6,
        out_specs=(VMEM, SMEM),
        scratch_shapes=[
            pltpu.VMEM((rows, block_len), jnp.bfloat16),
            pltpu.VMEM((rows, hid), jnp.bfloat16),
            pltpu.VMEM((rows, hid), jnp.bfloat16),
            pltpu.VMEM((classes, depth), jnp.bfloat16),
            pltpu.VMEM((classes, depth), jnp.bfloat16),
            pltpu.SMEM(need_blocks.shape, jnp.int32),
            pltpu.VMEM((height, width), jnp.float32),
            pltpu.VMEM((padded, 2 * depth), jnp.float32),
            pltpu.SemaphoreType.DMA((6,)),
        ],
        compiler_params=pltpu.CompilerParams(vmem_limit_bytes=4 * MIB),
        cost_estimate=pl.CostEstimate(flops=2 * MIB, bytes_accessed=MIB // 4, transcendentals=0),
        name="pack",
    )(*map(in_hbm, (features, w1_self, w1_nbr, w2_self.T, w2_nbr.T, need_blocks)))

    blocks = [packed] + [from_ahead(packed, "feat", step) for step in range(1, feats)]
    edges_one, edges_two = pl.pallas_call(
        functools.partial(load_kernel, 4),
        out_shape=(
            jax.ShapeDtypeStruct(edges_one.shape, jnp.int32),
            jax.ShapeDtypeStruct(edges_two.shape, jnp.int32),
        ),
        in_specs=[HBM, HBM, VMEM],
        out_specs=(VMEM, VMEM),
        scratch_shapes=[pltpu.SemaphoreType.DMA((5,))],
        compiler_params=pltpu.CompilerParams(vmem_limit_bytes=1 * MIB),
        cost_estimate=pl.CostEstimate(
            flops=100 * MIB, bytes_accessed=20 * MIB, transcendentals=0
        ),
        name="load",
    )(in_hbm(edges_one), in_hbm(edges_two), packed)

    self_term, mine = pl.pallas_call(
        functools.partial(first_kernel, rows, hid, classes),
        out_shape=(
            jax.ShapeDtypeStruct((padded, block_len), jnp.float32),
            jax.ShapeDtypeStruct((padded, block_len), jnp.bfloat16),
        ),
        in_specs=[VMEM] * 5,
        out_specs=(VMEM, VMEM),
        scratch_shapes=[
            pltpu.VMEM((feats, height, width), jnp.bfloat16),
            pltpu.VMEM((feats, padded, LANES), jnp.float32),
            pltpu.VMEM((2 * feats * height, hid), jnp.bfloat16),
        ],
        compiler_params=pltpu.CompilerParams(vmem_limit_bytes=16 * MIB),
        cost_estimate=pl.CostEstimate(
            flops=2 * 128 * block_len * block_len, bytes_accessed=4 * MIB, transcendentals=0
        ),
        name="first",
    )(*blocks, edges_one)

    def second(own, half, behind, fourth, *rest):
        return pl.pallas_call(
            functools.partial(second_kernel, classes),
            out_shape=(
                jax.ShapeDtypeStruct((1, block_len), jnp.float32),
                jax.ShapeDtypeStruct((nodes, 1, LANES), jnp.float32),
            ),
            in_specs=[VMEM] * 5 + [SMEM] + [VMEM] * 2,
            out_specs=(VMEM, VMEM),
            compiler_params=pltpu.CompilerParams(vmem_limit_bytes=4 * MIB),
            cost_estimate=pl.CostEstimate(
                flops=2 * 64 * 4 * block_len * block_len,
                bytes_accessed=16 * MIB,
                transcendentals=padded * block_len,
            ),
            name="second",
        )(own, half, behind, fourth, *rest)

    def with_offset(step, own, *rest):
        half = from_ahead(own, "node", nodes // 2)
        behind = from_ahead(own, "node", nodes - 1)
        fourth = from_ahead(own, "node", step)
        return second(own, half, behind, fourth, *rest)

    taken = (0, nodes // 2, nodes - 1)
    steps = [step for step in range(nodes) if step not in taken]
    loss, sums = lax.switch(
        number[0],
        [functools.partial(with_offset, step) for step in steps],
        mine,
        self_term,
        live_slots,
        edges_two,
        labels[None, :],
    )

    everyone = lax.all_to_all(sums, "node", 0, 0, tiled=True)
    mean_loss = jnp.sum(everyone[:, 0, 0]) / (block_len * nodes)
    return (loss[0], mean_loss)


def solution(mesh):
    return jax.shard_map(
        local,
        mesh=mesh,
        in_specs=(
            P("feat", "node"),
            P(None, "node"),
            P("feat", None),
            P("feat", None),
            P("node", None),
            P("node", None),
            P(None, "node"),
            P("feat", None),
            P("feat", None),
            P("node"),
        ),
        out_specs=(P("node"), P()),
        check_vma=False,
    )
```

```python
import functools

import jax
import jax.numpy as jnp
from jax import lax
from jax.experimental import pallas as pl
from jax.experimental.pallas import tpu as pltpu
from jax.sharding import PartitionSpec as P

FAN1 = 25
FAN2 = 10
LANES = 128
WORDS = 32
MIB = 1 << 20

VMEM = pl.BlockSpec(memory_space=pltpu.VMEM)
HBM = pl.BlockSpec(memory_space=pltpu.HBM)
SMEM = pl.BlockSpec(memory_space=pltpu.SMEM)


def in_hbm(value):
    return pltpu.with_memory_space_constraint(value, pltpu.HBM)


def from_ahead(value, axis, steps):
    count = lax.axis_size(axis)
    pairs = [(source, (source - steps) % count) for source in range(count)]
    return lax.ppermute(value, axis, pairs)


def pack_kernel(nodes, *refs):
    sources, (out_ref, off_ref), held, (scr, cat, sems) = refs[:6], refs[6:8], refs[8:14], refs[14:]
    copies = [
        pltpu.make_async_copy(source, place, sems.at[index])
        for index, (source, place) in enumerate(zip(sources, held))
    ]
    for copy in copies:
        copy.start()
    x_ref, ws_ref, wn_ref, us_ref, un_ref, need_ref = held
    rows, cols = x_ref.shape
    hid = ws_ref.shape[1]
    classes, depth = us_ref.shape
    spare = out_ref.shape[0] - rows
    bands = pl.cdiv(classes, spare)
    scr[rows:, :] = jnp.zeros((spare, scr.shape[1]), jnp.float32)
    for copy in copies:
        copy.wait()
    scr[:rows, :cols] = x_ref[...].astype(jnp.float32)
    scr[:rows, cols : cols + hid] = ws_ref[...].astype(jnp.float32)
    scr[:rows, cols + hid :] = wn_ref[...].astype(jnp.float32)
    cat[:classes, :depth] = us_ref[...].astype(jnp.float32)
    cat[:classes, depth:] = un_ref[...].astype(jnp.float32)
    for band in range(bands):
        first = band * spare
        count = min(spare, classes - first)
        scr[rows : rows + count, band * LANES : (band + 1) * LANES] = cat[first : first + count, :]
    out_ref[...] = scr[...].astype(jnp.bfloat16)
    offset = lax.rem(need_ref[0, 3] - lax.axis_index("node") + nodes, nodes)
    off_ref[0] = offset - 1 - (offset > nodes // 2).astype(jnp.int32)


def packed_bits(piece, first_bit):
    words = None
    for group in range(piece.shape[0] // WORDS):
        bits = piece[group * WORDS : (group + 1) * WORDS, :] << (first_bit + group)
        words = bits if words is None else words | bits
    return words


def load_kernel(e1_ref, e2_ref, after_ref, e1_out, bits_ref, held, sems):
    pieces = held.shape[0]
    rows = held.shape[1]
    base = e1_ref.shape[0]
    copies = [
        pltpu.make_async_copy(
            e2_ref.at[pl.ds(base + index * rows, rows)], held.at[index], sems.at[index]
        )
        for index in range(pieces)
    ]
    copies.append(pltpu.make_async_copy(e1_ref, e1_out, sems.at[pieces]))
    for copy in copies:
        copy.start()
    words = jnp.zeros(bits_ref.shape, jnp.int32)
    for index in range(pieces):
        copies[index].wait()
        words = words | packed_bits(held.at[index], index * (rows // WORDS))
    bits_ref[...] = words
    copies[pieces].wait()


def stream_kernel(z_ref, self_ref, e2_ref, total_ref, bits_ref, held, acc, sems):
    rows = held.shape[1]
    cols = z_ref.shape[1]
    pieces = cols // rows
    sources = [slot * pieces + index for slot in (0, 2, 3) for index in range(pieces)]
    copies = [
        pltpu.make_async_copy(e2_ref.at[pl.ds(source * rows, rows)], held.at[index], sems.at[index])
        for index, source in enumerate(sources)
    ]
    for copy in copies:
        copy.start()
    acc[...] = jnp.zeros_like(acc)

    def arrived(index):
        pltpu.make_async_copy(e2_ref.at[pl.ds(0, rows)], held.at[index], sems.at[index]).wait()
        return held.at[index]

    @pl.loop(0, pieces)
    def _(index):
        adjacency = arrived(index)[...].astype(jnp.float32).astype(jnp.bfloat16)
        own = z_ref[:, pl.ds(pl.multiple_of(index * rows, rows), rows)]
        acc[...] += jnp.dot(own, adjacency, preferred_element_type=jnp.float32)

    total_ref[...] = self_ref[...] + acc[...] / FAN2
    bits_ref[...] = jnp.zeros_like(bits_ref)

    @pl.loop(pieces, 3 * pieces)
    def _(index):
        slot = index // pieces - 1
        piece = arrived(index)
        bits_ref[slot] = bits_ref[slot] | packed_bits(piece, (index % pieces) * (rows // WORDS))


def first_kernel(
    rows, hid, classes, p0_ref, p1_ref, p2_ref, p3_ref, e_ref, self_ref, z_ref, blocks, w2, w1
):
    me = lax.axis_index("feat")
    feats, height, width = blocks.shape
    cols = width - 2 * hid
    spare = height - rows
    for step, ref in enumerate((p0_ref, p1_ref, p2_ref, p3_ref)):
        blocks[lax.rem(me + step, feats)] = ref[...]
    bands = pl.cdiv(classes, spare)
    for f in range(feats):
        for band in range(bands):
            count = min(spare, classes - band * spare)
            tail = blocks[f, :, band * LANES : (band + 1) * LANES].astype(jnp.float32)
            w2[f, band * spare : band * spare + count, :] = tail[rows : rows + count]
        w2[f, classes:, :] = jnp.zeros((w2.shape[1] - classes, LANES), jnp.float32)
    half = LANES // 2
    low = lax.broadcasted_iota(jnp.int32, (w2.shape[1], LANES), 1) < half
    selfs, nbrs = [], []
    for f in range(0, feats, 2):
        a, b = w2[f], w2[f + 1]
        selfs.append(jnp.where(low, a, pltpu.roll(b, half, 1)))
        nbrs.append(jnp.where(low, pltpu.roll(a, half, 1), b))
    project = jnp.concatenate(
        [jnp.concatenate(selfs, axis=1), jnp.concatenate(nbrs, axis=1)], axis=0
    ).astype(jnp.bfloat16)
    inputs = blocks[:, :, :cols].reshape(feats * height, cols)
    w1[: feats * height, :] = blocks[:, :, cols : cols + hid].reshape(feats * height, hid)
    w1[feats * height :, :] = blocks[:, :, cols + hid :].reshape(feats * height, hid)
    weights = w1[...]
    padded = w2.shape[1]
    chunk = 256
    for first in range(0, cols, chunk):
        part = slice(first, first + chunk)
        adjacency = e_ref[:, part].astype(jnp.float32).astype(jnp.bfloat16)
        nbr = jnp.dot(inputs, adjacency, preferred_element_type=jnp.float32) / FAN1
        stacked = jnp.concatenate([inputs[:, part], nbr.astype(jnp.bfloat16)], axis=0)
        before = lax.dot_general(
            weights, stacked, (((0,), (0,)), ((), ())), preferred_element_type=jnp.float32
        )
        hidden = jnp.maximum(before, 0.0).astype(jnp.bfloat16)
        both = jnp.dot(project, hidden, preferred_element_type=jnp.float32)
        self_ref[:, part] = both[:padded]
        z_ref[:, part] = both[padded:].astype(jnp.bfloat16)


def second_kernel(
    classes, z1_ref, z2_ref, z3_ref, total_ref, live_ref, b1_ref, b23_ref, label_ref, loss_ref, sum_ref, zs
):
    padded, cols = total_ref.shape
    chunk = 256
    group = lax.broadcasted_iota(jnp.int32, (1, cols), 1) // WORDS
    scale = jnp.ones((1, cols), jnp.float32)
    for bit in range(5):
        scale = scale * jnp.where((group >> bit) % 2 == 1, 2.0 ** -(1 << bit), 1.0)
    scale = jnp.where(group == 31, -scale, scale)
    for slot, ref in enumerate((z1_ref, z2_ref, z3_ref)):
        used = jnp.where(live_ref[0, slot + 1] == 1, scale, 0.0)
        zs[:, slot * cols : (slot + 1) * cols] = (ref[...].astype(jnp.float32) * used).astype(
            jnp.bfloat16
        )
    class_ids = lax.broadcasted_iota(jnp.int32, (padded, chunk), 0)
    summed = jnp.zeros((1, chunk), jnp.float32)
    for first in range(0, cols, chunk):
        part = slice(first, first + chunk)
        term = jnp.zeros((padded, chunk), jnp.float32)
        for slot, words in enumerate((b1_ref[:, part], b23_ref[0, :, part], b23_ref[1, :, part])):
            planes = []
            for bit in range(32):
                mask = (1 << bit) if bit < 31 else -(1 << 31)
                planes.append((words & jnp.int32(mask)).astype(jnp.float32).astype(jnp.bfloat16))
            adjacency = jnp.concatenate(planes, axis=0)
            term = term + jnp.dot(
                zs[:, slot * cols : (slot + 1) * cols], adjacency, preferred_element_type=jnp.float32
            )
        logits = total_ref[:, part] + term / FAN2
        powers = jnp.where(class_ids < classes, jnp.exp(logits), 0.0)
        picked = jnp.where(class_ids == label_ref[:, part], logits, 0.0)
        loss = jnp.log(jnp.sum(powers, 0, keepdims=True)) - jnp.sum(picked, 0, keepdims=True)
        loss_ref[:, part] = loss
        summed = summed + loss
    mean = jnp.sum(summed, keepdims=True) / (cols * sum_ref.shape[0])
    sum_ref[...] = jnp.broadcast_to(mean.reshape(1, 1, 1), sum_ref.shape)


def local(
    features,
    edges_one,
    w1_self,
    w1_nbr,
    need_blocks,
    live_slots,
    edges_two,
    w2_self,
    w2_nbr,
    labels,
):
    rows, block_len = features.shape
    hid = w1_self.shape[1]
    depth, classes = w2_self.shape
    nodes = lax.axis_size("node")
    feats = lax.axis_size("feat")
    height = pl.cdiv(rows, 8) * 8
    width = block_len + 2 * hid
    padded = pl.cdiv(classes, 16) * 16

    packed, number = pl.pallas_call(
        functools.partial(pack_kernel, nodes),
        out_shape=(
            jax.ShapeDtypeStruct((height, width), jnp.bfloat16),
            jax.ShapeDtypeStruct((1,), jnp.int32),
        ),
        in_specs=[HBM] * 6,
        out_specs=(VMEM, SMEM),
        scratch_shapes=[
            pltpu.VMEM((rows, block_len), jnp.bfloat16),
            pltpu.VMEM((rows, hid), jnp.bfloat16),
            pltpu.VMEM((rows, hid), jnp.bfloat16),
            pltpu.VMEM((classes, depth), jnp.bfloat16),
            pltpu.VMEM((classes, depth), jnp.bfloat16),
            pltpu.SMEM(need_blocks.shape, jnp.int32),
            pltpu.VMEM((height, width), jnp.float32),
            pltpu.VMEM((padded, 2 * depth), jnp.float32),
            pltpu.SemaphoreType.DMA((6,)),
        ],
        compiler_params=pltpu.CompilerParams(vmem_limit_bytes=4 * MIB),
        cost_estimate=pl.CostEstimate(flops=2 * MIB, bytes_accessed=MIB // 4, transcendentals=0),
        name="pack",
    )(*map(in_hbm, (features, w1_self, w1_nbr, w2_self.T, w2_nbr.T, need_blocks)))

    blocks = [packed] + [from_ahead(packed, "feat", step) for step in range(1, feats)]
    words = block_len // 32
    edges_one, bits_one = pl.pallas_call(
        load_kernel,
        out_shape=(
            jax.ShapeDtypeStruct(edges_one.shape, jnp.int32),
            jax.ShapeDtypeStruct((words, block_len), jnp.int32),
        ),
        in_specs=[HBM, HBM, VMEM],
        out_specs=(VMEM, VMEM),
        scratch_shapes=[
            pltpu.VMEM((4, block_len // 4, block_len), jnp.int32),
            pltpu.SemaphoreType.DMA((5,)),
        ],
        compiler_params=pltpu.CompilerParams(vmem_limit_bytes=8 * MIB),
        cost_estimate=pl.CostEstimate(flops=100 * MIB, bytes_accessed=8 * MIB, transcendentals=0),
        name="load",
    )(in_hbm(edges_one), in_hbm(edges_two), packed)

    self_term, mine = pl.pallas_call(
        functools.partial(first_kernel, rows, hid, classes),
        out_shape=(
            jax.ShapeDtypeStruct((padded, block_len), jnp.float32),
            pltpu.VMEM((padded, block_len), jnp.bfloat16),
        ),
        in_specs=[VMEM] * 5,
        out_specs=(VMEM, VMEM),
        scratch_shapes=[
            pltpu.VMEM((feats, height, width), jnp.bfloat16),
            pltpu.VMEM((feats, padded, LANES), jnp.float32),
            pltpu.VMEM((2 * feats * height, hid), jnp.bfloat16),
        ],
        compiler_params=pltpu.CompilerParams(vmem_limit_bytes=16 * MIB),
        cost_estimate=pl.CostEstimate(
            flops=2 * 128 * block_len * block_len, bytes_accessed=4 * MIB, transcendentals=0
        ),
        name="first",
    )(*blocks, edges_one)

    half = from_ahead(mine, "node", nodes // 2)
    behind = from_ahead(mine, "node", nodes - 1)

    def with_offset(step, own, self_term, edges_two):
        fourth = from_ahead(own, "node", step)
        total, bits_rest = pl.pallas_call(
            stream_kernel,
            out_shape=(
                jax.ShapeDtypeStruct((padded, block_len), jnp.float32),
                jax.ShapeDtypeStruct((2, words, block_len), jnp.int32),
            ),
            in_specs=[VMEM, VMEM, HBM],
            out_specs=(VMEM, VMEM),
            scratch_shapes=[
                pltpu.VMEM((12, block_len // 4, block_len), jnp.int32),
                pltpu.VMEM((padded, block_len), jnp.float32),
                pltpu.SemaphoreType.DMA((12,)),
            ],
            compiler_params=pltpu.CompilerParams(vmem_limit_bytes=24 * MIB),
            cost_estimate=pl.CostEstimate(
                flops=100 * MIB, bytes_accessed=12 * MIB, transcendentals=0
            ),
            name="stream",
        )(own, self_term, in_hbm(edges_two))
        return fourth, total, bits_rest

    taken = (0, nodes // 2, nodes - 1)
    steps = [step for step in range(nodes) if step not in taken]
    fourth, total, bits_rest = lax.switch(
        number[0],
        [functools.partial(with_offset, step) for step in steps],
        mine,
        self_term,
        edges_two,
    )

    loss, sums = pl.pallas_call(
        functools.partial(second_kernel, classes),
        out_shape=(
            jax.ShapeDtypeStruct((1, block_len), jnp.float32),
            jax.ShapeDtypeStruct((nodes, 1, LANES), jnp.float32),
        ),
        in_specs=[VMEM] * 4 + [SMEM] + [VMEM] * 3,
        out_specs=(VMEM, VMEM),
        scratch_shapes=[pltpu.VMEM((padded, 3 * block_len), jnp.bfloat16)],
        compiler_params=pltpu.CompilerParams(vmem_limit_bytes=16 * MIB),
        cost_estimate=pl.CostEstimate(
            flops=2 * 64 * 3 * block_len * block_len,
            bytes_accessed=2 * MIB,
            transcendentals=padded * block_len,
        ),
        name="second",
    )(half, behind, fourth, total, live_slots, bits_one, bits_rest, labels[None, :])

    everyone = lax.all_to_all(sums, "node", 0, 0, tiled=True)
    mean_loss = jnp.sum(everyone[:, 0, 0])
    return (loss[0], mean_loss)


def solution(mesh):
    return jax.shard_map(
        local,
        mesh=mesh,
        in_specs=(
            P("feat", "node"),
            P(None, "node"),
            P("feat", None),
            P("feat", None),
            P("node", None),
            P("node", None),
            P(None, "node"),
            P("feat", None),
            P("feat", None),
            P("node"),
        ),
        out_specs=(P("node"), P()),
        check_vma=False,
    )
```

```python
import functools

import jax
import jax.numpy as jnp
from jax import lax
from jax.experimental import pallas as pl
from jax.experimental.pallas import tpu as pltpu
from jax.sharding import PartitionSpec as P

FAN1 = 25
FAN2 = 10
LANES = 128
WORDS = 32
MIB = 1 << 20

VMEM = pl.BlockSpec(memory_space=pltpu.VMEM)
HBM = pl.BlockSpec(memory_space=pltpu.HBM)
SMEM = pl.BlockSpec(memory_space=pltpu.SMEM)


def in_hbm(value):
    return pltpu.with_memory_space_constraint(value, pltpu.HBM)


def from_ahead(value, axis, steps):
    count = lax.axis_size(axis)
    pairs = [(source, (source - steps) % count) for source in range(count)]
    return lax.ppermute(value, axis, pairs)


def pack_kernel(nodes, *refs):
    sources, (out_ref, off_ref), held, (scr, cat, sems) = refs[:6], refs[6:8], refs[8:14], refs[14:]
    copies = [
        pltpu.make_async_copy(source, place, sems.at[index])
        for index, (source, place) in enumerate(zip(sources, held))
    ]
    for copy in copies:
        copy.start()
    x_ref, ws_ref, wn_ref, us_ref, un_ref, need_ref = held
    rows, cols = x_ref.shape
    hid = ws_ref.shape[1]
    classes, depth = us_ref.shape
    height = out_ref.shape[0]
    side = cols + 2 * hid
    scr[rows:, :] = jnp.zeros((height - rows, side), jnp.float32)
    cat[...] = jnp.zeros_like(cat)
    for copy in copies:
        copy.wait()
    scr[:rows, :cols] = x_ref[...].astype(jnp.float32)
    scr[:rows, cols : cols + hid] = ws_ref[...].astype(jnp.float32)
    scr[:rows, cols + hid :] = wn_ref[...].astype(jnp.float32)
    cat[:classes, :depth] = us_ref[...].astype(jnp.float32)
    cat[LANES // 2 : LANES // 2 + classes, :depth] = un_ref[...].astype(jnp.float32)
    by_unit = cat[...].T
    out_ref[:, :side] = scr[...].astype(jnp.bfloat16)
    for piece in range(depth // height):
        place = slice(side + piece * LANES, side + (piece + 1) * LANES)
        out_ref[:, place] = by_unit[piece * height : (piece + 1) * height].astype(jnp.bfloat16)
    offset = lax.rem(need_ref[0, 3] - lax.axis_index("node") + nodes, nodes)
    off_ref[0] = offset - 1 - (offset > nodes // 2).astype(jnp.int32)


def packed_bits(piece, first_bit):
    words = None
    for group in range(piece.shape[0] // WORDS):
        bits = piece[group * WORDS : (group + 1) * WORDS, :] << (first_bit + group)
        words = bits if words is None else words | bits
    return words


def load_kernel(e1_ref, e2_ref, after_ref, e1_out, bits_ref, held, sems):
    pieces, rows = held.shape[0] // 2, held.shape[1]
    base = e1_ref.shape[0]
    copies = []
    for index in range(2 * pieces):
        ref, first = (e1_ref, 0) if index < pieces else (e2_ref, base)
        source = ref.at[pl.ds(first + index % pieces * rows, rows)]
        copies.append(pltpu.make_async_copy(source, held.at[index], sems.at[index]))
    for copy in copies:
        copy.start()
    for index in range(pieces):
        copies[index].wait()
        e1_out[index * rows : (index + 1) * rows, :] = (
            held[index].astype(jnp.float32).astype(jnp.bfloat16)
        )
    words = jnp.zeros(bits_ref.shape, jnp.int32)
    for index in range(pieces):
        copies[pieces + index].wait()
        words = words | packed_bits(held.at[pieces + index], index * (rows // WORDS))
    bits_ref[...] = words


def stream_kernel(z_ref, self_ref, e2_ref, total_ref, bits_ref, held, acc, sems):
    rows = held.shape[1]
    cols = z_ref.shape[1]
    pieces = cols // rows
    sources = [slot * pieces + index for slot in (0, 2) for index in range(pieces)]
    copies = [
        pltpu.make_async_copy(e2_ref.at[pl.ds(source * rows, rows)], held.at[index], sems.at[index])
        for index, source in enumerate(sources)
    ]
    for copy in copies:
        copy.start()
    acc[...] = jnp.zeros_like(acc)

    def arrived(index):
        pltpu.make_async_copy(e2_ref.at[pl.ds(0, rows)], held.at[index], sems.at[index]).wait()
        return held.at[index]

    @pl.loop(0, pieces)
    def _(index):
        adjacency = arrived(index)[...].astype(jnp.float32).astype(jnp.bfloat16)
        own = z_ref[:, pl.ds(pl.multiple_of(index * rows, rows), rows)]
        acc[...] += jnp.dot(own, adjacency, preferred_element_type=jnp.float32)

    total_ref[...] = self_ref[...] + acc[...] / FAN2
    bits_ref[...] = jnp.zeros_like(bits_ref)

    @pl.loop(pieces, 2 * pieces)
    def _(index):
        first_bit = (index - pieces) * (rows // WORDS)
        bits_ref[...] = bits_ref[...] | packed_bits(arrived(index), first_bit)


def first_kernel(
    hid, depth, p0_ref, p1_ref, p2_ref, p3_ref, e_ref, self_ref, z_ref, send_ref, own_ref, x, w1, w2
):
    me = lax.axis_index("feat")
    height = p0_ref.shape[0]
    cols = x.shape[1]
    feats = x.shape[0] // height
    padded = z_ref.shape[0]
    for step, ref in enumerate((p0_ref, p1_ref, p2_ref, p3_ref)):
        place = lax.rem(me + step, feats)
        rows = pl.ds(pl.multiple_of(place * height, height), height)
        x[rows, :] = ref[:, :cols]
        w1[rows, :] = ref[:, cols : cols + hid]
        below = pl.ds(pl.multiple_of((feats + place) * height, height), height)
        w1[below, :] = ref[:, cols + hid : cols + 2 * hid]
        for piece in range(depth // height):
            units = pl.ds(pl.multiple_of(place * depth + piece * height, height), height)
            lanes = slice(cols + 2 * hid + piece * LANES, cols + 2 * hid + (piece + 1) * LANES)
            w2[units, :] = ref[:, lanes]
    inputs = x[...]
    weights = w1[...].astype(jnp.float32).T.astype(jnp.bfloat16)
    project = w2[...].astype(jnp.float32).T.astype(jnp.bfloat16)
    chunk = 256
    for first in range(0, cols, chunk):
        part = slice(first, first + chunk)
        nbr = jnp.dot(inputs, e_ref[:, part], preferred_element_type=jnp.float32) / FAN1
        stacked = jnp.concatenate([inputs[:, part], nbr.astype(jnp.bfloat16)], axis=0)
        before = jnp.dot(weights, stacked, preferred_element_type=jnp.float32)
        hidden = jnp.maximum(before, 0.0).astype(jnp.bfloat16)
        both = jnp.dot(project, hidden, preferred_element_type=jnp.float32)
        self_ref[:, part] = both[:padded]
        z = both[LANES // 2 : LANES // 2 + padded].astype(jnp.bfloat16)
        z_ref[:, part] = z
        send_ref[:, part] = z
        own_ref[:, part] = z


def second_kernel(
    classes,
    z1_ref,
    z2_ref,
    z3_hbm,
    total_ref,
    live_ref,
    b1_ref,
    b2_ref,
    e2_ref,
    label_ref,
    loss_ref,
    sum_ref,
    zs,
    z3_ref,
    held,
    acc,
    sems,
):
    padded, cols = total_ref.shape
    pieces, rows = held.shape[0], held.shape[1]
    fetch = pltpu.make_async_copy(z3_hbm, z3_ref, sems.at[pieces])
    fetch.start()
    copies = [
        pltpu.make_async_copy(
            e2_ref.at[pl.ds(3 * cols + index * rows, rows)], held.at[index], sems.at[index]
        )
        for index in range(pieces)
    ]
    for copy in copies:
        copy.start()
    chunk = 256
    group = lax.broadcasted_iota(jnp.int32, (1, cols), 1) // WORDS
    scale = jnp.ones((1, cols), jnp.float32)
    for bit in range(5):
        scale = scale * jnp.where((group >> bit) % 2 == 1, 2.0 ** -(1 << bit), 1.0)
    scale = jnp.where(group == 31, -scale, scale)
    for slot, ref in enumerate((z1_ref, z2_ref)):
        used = jnp.where(live_ref[0, slot + 1] == 1, scale, 0.0)
        zs[:, slot * cols : (slot + 1) * cols] = (ref[...].astype(jnp.float32) * used).astype(
            jnp.bfloat16
        )
    for first in range(0, cols, chunk):
        part = slice(first, first + chunk)
        planes = []
        for words in (b1_ref[:, part], b2_ref[:, part]):
            for bit in range(32):
                mask = (1 << bit) if bit < 31 else -(1 << 31)
                planes.append((words & jnp.int32(mask)).astype(jnp.float32).astype(jnp.bfloat16))
        adjacency = jnp.concatenate(planes, axis=0)
        acc[:, part] = jnp.dot(zs[...], adjacency, preferred_element_type=jnp.float32)
    fetch.wait()
    for copy in copies:
        copy.wait()
    live = jnp.where(live_ref[0, 3] == 1, 1.0, 0.0)
    fourth = (z3_ref[...].astype(jnp.float32) * live).astype(jnp.bfloat16)
    class_ids = lax.broadcasted_iota(jnp.int32, (padded, chunk), 0)
    summed = jnp.zeros((1, chunk), jnp.float32)
    for first in range(0, cols, chunk):
        part = slice(first, first + chunk)
        adjacency = held[:, :, part].reshape(cols, chunk)
        adjacency = adjacency.astype(jnp.float32).astype(jnp.bfloat16)
        term = acc[:, part] + jnp.dot(fourth, adjacency, preferred_element_type=jnp.float32)
        logits = total_ref[:, part] + term / FAN2
        powers = jnp.where(class_ids < classes, jnp.exp(logits), 0.0)
        picked = jnp.where(class_ids == label_ref[:, part], logits, 0.0)
        loss = jnp.log(jnp.sum(powers, 0, keepdims=True)) - jnp.sum(picked, 0, keepdims=True)
        loss_ref[:, part] = loss
        summed = summed + loss
    mean = jnp.sum(summed, keepdims=True) / (cols * sum_ref.shape[0])
    sum_ref[...] = jnp.broadcast_to(mean.reshape(1, 1, 1), sum_ref.shape)


def local(
    features,
    edges_one,
    w1_self,
    w1_nbr,
    need_blocks,
    live_slots,
    edges_two,
    w2_self,
    w2_nbr,
    labels,
):
    rows, block_len = features.shape
    hid = w1_self.shape[1]
    depth, classes = w2_self.shape
    nodes = lax.axis_size("node")
    feats = lax.axis_size("feat")
    height = pl.cdiv(rows, 8) * 8
    width = block_len + 2 * hid + depth // height * LANES
    padded = pl.cdiv(classes, 16) * 16

    packed, number = pl.pallas_call(
        functools.partial(pack_kernel, nodes),
        out_shape=(
            jax.ShapeDtypeStruct((height, width), jnp.bfloat16),
            jax.ShapeDtypeStruct((1,), jnp.int32),
        ),
        in_specs=[HBM] * 6,
        out_specs=(VMEM, SMEM),
        scratch_shapes=[
            pltpu.VMEM((rows, block_len), jnp.bfloat16),
            pltpu.VMEM((rows, hid), jnp.bfloat16),
            pltpu.VMEM((rows, hid), jnp.bfloat16),
            pltpu.VMEM((classes, depth), jnp.bfloat16),
            pltpu.VMEM((classes, depth), jnp.bfloat16),
            pltpu.SMEM(need_blocks.shape, jnp.int32),
            pltpu.VMEM((height, block_len + 2 * hid), jnp.float32),
            pltpu.VMEM((LANES, LANES), jnp.float32),
            pltpu.SemaphoreType.DMA((6,)),
        ],
        compiler_params=pltpu.CompilerParams(vmem_limit_bytes=4 * MIB),
        cost_estimate=pl.CostEstimate(flops=2 * MIB, bytes_accessed=MIB // 4, transcendentals=0),
        name="pack",
    )(*map(in_hbm, (features, w1_self, w1_nbr, w2_self.T, w2_nbr.T, need_blocks)))

    blocks = [packed] + [from_ahead(packed, "feat", step) for step in range(1, feats)]
    words = block_len // 32
    edges_one, bits_one = pl.pallas_call(
        load_kernel,
        out_shape=(
            jax.ShapeDtypeStruct(edges_one.shape, jnp.bfloat16),
            jax.ShapeDtypeStruct((words, block_len), jnp.int32),
        ),
        in_specs=[HBM, HBM, VMEM],
        out_specs=(VMEM, VMEM),
        scratch_shapes=[
            pltpu.VMEM((8, block_len // 4, block_len), jnp.int32),
            pltpu.SemaphoreType.DMA((8,)),
        ],
        compiler_params=pltpu.CompilerParams(vmem_limit_bytes=12 * MIB),
        cost_estimate=pl.CostEstimate(flops=100 * MIB, bytes_accessed=8 * MIB, transcendentals=0),
        name="load",
    )(in_hbm(edges_one), in_hbm(edges_two), packed)

    self_term, mine, send, own = pl.pallas_call(
        functools.partial(first_kernel, hid, depth),
        out_shape=(
            jax.ShapeDtypeStruct((padded, block_len), jnp.float32),
            jax.ShapeDtypeStruct((padded, block_len), jnp.bfloat16),
            jax.ShapeDtypeStruct((padded, block_len), jnp.bfloat16),
            jax.ShapeDtypeStruct((padded, block_len), jnp.bfloat16),
        ),
        in_specs=[VMEM] * 5,
        out_specs=(VMEM,) * 4,
        scratch_shapes=[
            pltpu.VMEM((feats * height, block_len), jnp.bfloat16),
            pltpu.VMEM((2 * feats * height, hid), jnp.bfloat16),
            pltpu.VMEM((feats * depth, LANES), jnp.bfloat16),
        ],
        compiler_params=pltpu.CompilerParams(vmem_limit_bytes=16 * MIB),
        cost_estimate=pl.CostEstimate(
            flops=2 * 128 * block_len * block_len, bytes_accessed=4 * MIB, transcendentals=0
        ),
        name="first",
    )(*blocks, edges_one)

    half = from_ahead(mine, "node", nodes // 2)
    behind = from_ahead(mine, "node", nodes - 1)

    def with_offset(step, send, own, self_term, edges_two):
        fourth = from_ahead(send, "node", step)
        total, bits_two = pl.pallas_call(
            stream_kernel,
            out_shape=(
                jax.ShapeDtypeStruct((padded, block_len), jnp.float32),
                jax.ShapeDtypeStruct((words, block_len), jnp.int32),
            ),
            in_specs=[VMEM, VMEM, HBM],
            out_specs=(VMEM, VMEM),
            scratch_shapes=[
                pltpu.VMEM((8, block_len // 4, block_len), jnp.int32),
                pltpu.VMEM((padded, block_len), jnp.float32),
                pltpu.SemaphoreType.DMA((8,)),
            ],
            compiler_params=pltpu.CompilerParams(vmem_limit_bytes=12 * MIB),
            cost_estimate=pl.CostEstimate(
                flops=100 * MIB, bytes_accessed=8 * MIB, transcendentals=0
            ),
            name="stream",
        )(own, self_term, in_hbm(edges_two))
        return fourth, total, bits_two

    taken = (0, nodes // 2, nodes - 1)
    steps = [step for step in range(nodes) if step not in taken]
    fourth, total, bits_two = lax.switch(
        number[0],
        [functools.partial(with_offset, step) for step in steps],
        send,
        own,
        self_term,
        edges_two,
    )

    loss, sums = pl.pallas_call(
        functools.partial(second_kernel, classes),
        out_shape=(
            jax.ShapeDtypeStruct((1, block_len), jnp.float32),
            jax.ShapeDtypeStruct((nodes, 1, LANES), jnp.float32),
        ),
        in_specs=[VMEM, VMEM, HBM, VMEM, SMEM, VMEM, VMEM, HBM, VMEM],
        out_specs=(VMEM, VMEM),
        scratch_shapes=[
            pltpu.VMEM((padded, 2 * block_len), jnp.bfloat16),
            pltpu.VMEM((padded, block_len), jnp.bfloat16),
            pltpu.VMEM((4, block_len // 4, block_len), jnp.int32),
            pltpu.VMEM((padded, block_len), jnp.float32),
            pltpu.SemaphoreType.DMA((5,)),
        ],
        compiler_params=pltpu.CompilerParams(vmem_limit_bytes=16 * MIB),
        cost_estimate=pl.CostEstimate(
            flops=2 * 64 * 3 * block_len * block_len,
            bytes_accessed=2 * MIB,
            transcendentals=padded * block_len,
        ),
        name="second",
    )(
        half,
        behind,
        in_hbm(fourth),
        total,
        live_slots,
        bits_one,
        bits_two,
        in_hbm(edges_two),
        labels[None, :],
    )

    everyone = lax.all_to_all(sums, "node", 0, 0, tiled=True)
    mean_loss = jnp.sum(everyone[:, 0, 0])
    return (loss[0], mean_loss)


def solution(mesh):
    return jax.shard_map(
        local,
        mesh=mesh,
        in_specs=(
            P("feat", "node"),
            P(None, "node"),
            P("feat", None),
            P("feat", None),
            P("node", None),
            P("node", None),
            P(None, "node"),
            P("feat", None),
            P("feat", None),
            P("node"),
        ),
        out_specs=(P("node"), P()),
        check_vma=False,
    )
```

```python
import functools

import jax
import jax.numpy as jnp
from jax import lax
from jax.experimental import pallas as pl
from jax.experimental.pallas import tpu as pltpu
from jax.sharding import PartitionSpec as P

FAN1 = 25
FAN2 = 10
LANES = 128
WORDS = 32
MIB = 1 << 20

VMEM = pl.BlockSpec(memory_space=pltpu.VMEM)
HBM = pl.BlockSpec(memory_space=pltpu.HBM)
SMEM = pl.BlockSpec(memory_space=pltpu.SMEM)


def in_hbm(value):
    return pltpu.with_memory_space_constraint(value, pltpu.HBM)


def from_ahead(value, axis, steps):
    count = lax.axis_size(axis)
    pairs = [(source, (source - steps) % count) for source in range(count)]
    return lax.ppermute(value, axis, pairs)


def pack_kernel(*refs):
    sources, (out_ref, edges_ref), held, (scr, cat, sems) = refs[:6], refs[6:8], refs[8:13], refs[13:]
    copies = [
        pltpu.make_async_copy(source, place, sems.at[index])
        for index, (source, place) in enumerate(zip(sources[:5], held))
    ]
    ahead = sources[5].at[pl.ds(0, edges_ref.shape[0])]
    copies.append(pltpu.make_async_copy(ahead, edges_ref, sems.at[5]))
    for copy in copies:
        copy.start()
    x_ref, ws_ref, wn_ref, us_ref, un_ref = held
    rows, cols = x_ref.shape
    hid = ws_ref.shape[1]
    classes, depth = us_ref.shape
    height = out_ref.shape[0]
    side = cols + 2 * hid
    scr[rows:, :] = jnp.zeros((height - rows, side), jnp.float32)
    cat[...] = jnp.zeros_like(cat)
    for copy in copies[:5]:
        copy.wait()
    scr[:rows, :cols] = x_ref[...].astype(jnp.float32)
    scr[:rows, cols : cols + hid] = ws_ref[...].astype(jnp.float32)
    scr[:rows, cols + hid :] = wn_ref[...].astype(jnp.float32)
    cat[:classes, :depth] = us_ref[...].astype(jnp.float32)
    cat[LANES // 2 : LANES // 2 + classes, :depth] = un_ref[...].astype(jnp.float32)
    by_unit = cat[...].T
    out_ref[:, :side] = scr[...].astype(jnp.bfloat16)
    for piece in range(depth // height):
        place = slice(side + piece * LANES, side + (piece + 1) * LANES)
        out_ref[:, place] = by_unit[piece * height : (piece + 1) * height].astype(jnp.bfloat16)
    copies[5].wait()


def packed_bits(piece, first_bit):
    words = None
    for group in range(piece.shape[0] // WORDS):
        bits = piece[group * WORDS : (group + 1) * WORDS, :] << (first_bit + group)
        words = bits if words is None else words | bits
    return words


def load_kernel(
    nodes, e1_ref, ready_ref, e2_ref, need_ref, live_ref, e1_out, bits_ref, number_ref, need, live, held, sems
):
    pieces, rows = bits_ref.shape[0] * 4, held.shape[1]
    cols = e1_out.shape[0]
    done = ready_ref.shape[0]
    sources = [e1_ref.at[pl.ds(first, rows)] for first in range(done, cols, rows)]
    before = len(sources)
    for slot in (1, 3):
        sources += [e2_ref.at[pl.ds(first, rows)] for first in range(slot * cols, (slot + 1) * cols, rows)]
    copies = [
        pltpu.make_async_copy(source, held.at[index], sems.at[index])
        for index, source in enumerate(sources)
    ]
    small = [
        pltpu.make_async_copy(need_ref, need, sems.at[len(sources)]),
        pltpu.make_async_copy(live_ref, live, sems.at[len(sources) + 1]),
    ]
    for copy in small + copies:
        copy.start()
    e1_out[:done, :] = ready_ref[...].astype(jnp.float32).astype(jnp.bfloat16)
    for copy in small:
        copy.wait()
    offset = lax.rem(need[0, 3] - lax.axis_index("node") + nodes, nodes)
    number_ref[0] = offset - 1 - (offset > nodes // 2).astype(jnp.int32)
    for index in range(before):
        copies[index].wait()
        first = done + index * rows
        e1_out[first : first + rows, :] = held[index].astype(jnp.float32).astype(jnp.bfloat16)
    per_slot = cols // rows
    for place, slot in enumerate((1, 3)):
        words = jnp.zeros(bits_ref.shape[1:], jnp.int32)
        for index in range(per_slot):
            at = before + place * per_slot + index
            copies[at].wait()
            words = words | packed_bits(held.at[at], index * (rows // WORDS))
        bits_ref[place] = jnp.where(live[0, slot] == 1, words, 0)


def stream_kernel(z_ref, self_ref, e2_ref, live_ref, total_ref, bits_ref, held, acc, live, sems):
    rows = held.shape[1]
    cols = z_ref.shape[1]
    pieces = cols // rows
    sources = [slot * pieces + index for slot in (0, 2) for index in range(pieces)]
    copies = [
        pltpu.make_async_copy(e2_ref.at[pl.ds(source * rows, rows)], held.at[index], sems.at[index])
        for index, source in enumerate(sources)
    ]
    copies.append(pltpu.make_async_copy(live_ref, live, sems.at[2 * pieces]))
    for copy in copies:
        copy.start()
    acc[...] = jnp.zeros_like(acc)

    def arrived(index):
        pltpu.make_async_copy(e2_ref.at[pl.ds(0, rows)], held.at[index], sems.at[index]).wait()
        return held.at[index]

    @pl.loop(0, pieces)
    def _(index):
        adjacency = arrived(index)[...].astype(jnp.float32).astype(jnp.bfloat16)
        own = z_ref[:, pl.ds(pl.multiple_of(index * rows, rows), rows)]
        acc[...] += jnp.dot(own, adjacency, preferred_element_type=jnp.float32)

    total_ref[...] = self_ref[...] + acc[...] / FAN2
    bits_ref[...] = jnp.zeros_like(bits_ref)

    @pl.loop(pieces, 2 * pieces)
    def _(index):
        first_bit = (index - pieces) * (rows // WORDS)
        bits_ref[...] = bits_ref[...] | packed_bits(arrived(index), first_bit)

    copies[-1].wait()
    bits_ref[...] = jnp.where(live[0, 2] == 1, bits_ref[...], 0)


def first_kernel(
    hid, depth, p0_ref, p2_ref, p3_ref, p1_ref, e_ref, after_ref, self_ref, z_ref, send_ref, own_ref, x, w1, w2
):
    me = lax.axis_index("feat")
    height = p0_ref.shape[0]
    cols = x.shape[1]
    feats = x.shape[0] // height
    padded = z_ref.shape[0]
    for step, ref in enumerate((p0_ref, p1_ref, p2_ref, p3_ref)):
        place = lax.rem(me + step, feats)
        rows = pl.ds(pl.multiple_of(place * height, height), height)
        x[rows, :] = ref[:, :cols]
        w1[rows, :] = ref[:, cols : cols + hid]
        below = pl.ds(pl.multiple_of((feats + place) * height, height), height)
        w1[below, :] = ref[:, cols + hid : cols + 2 * hid]
        for piece in range(depth // height):
            units = pl.ds(pl.multiple_of(place * depth + piece * height, height), height)
            lanes = slice(cols + 2 * hid + piece * LANES, cols + 2 * hid + (piece + 1) * LANES)
            w2[units, :] = ref[:, lanes]
    inputs = x[...]
    weights = w1[...].astype(jnp.float32).T.astype(jnp.bfloat16)
    project = w2[...].astype(jnp.float32).T.astype(jnp.bfloat16)
    group = lax.broadcasted_iota(jnp.int32, (1, cols), 1) // WORDS
    scale = jnp.ones((1, cols), jnp.float32)
    for bit in range(5):
        scale = scale * jnp.where((group >> bit) % 2 == 1, 2.0 ** -(1 << bit), 1.0)
    scale = jnp.where(group == 31, -scale, scale)
    chunk = 256
    for first in range(0, cols, chunk):
        part = slice(first, first + chunk)
        nbr = jnp.dot(inputs, e_ref[:, part], preferred_element_type=jnp.float32) / FAN1
        stacked = jnp.concatenate([inputs[:, part], nbr.astype(jnp.bfloat16)], axis=0)
        before = jnp.dot(weights, stacked, preferred_element_type=jnp.float32)
        hidden = jnp.maximum(before, 0.0).astype(jnp.bfloat16)
        both = jnp.dot(project, hidden, preferred_element_type=jnp.float32)
        self_ref[:, part] = both[:padded]
        z = both[LANES // 2 : LANES // 2 + padded]
        own_ref[:, part] = z.astype(jnp.bfloat16)
        scaled = (z * scale[:, part]).astype(jnp.bfloat16)
        z_ref[:, part] = scaled
        send_ref[:, part] = scaled


def second_kernel(
    classes, z2_ref, z1_ref, z3_hbm, total_ref, b13_ref, b2_ref, label_ref, loss_ref, sum_ref, z3_ref, acc, sem
):
    padded, cols = total_ref.shape
    fetch = pltpu.make_async_copy(z3_hbm, z3_ref, sem)
    fetch.start()
    chunk = 256

    def edges(words):
        planes = []
        for bit in range(32):
            mask = (1 << bit) if bit < 31 else -(1 << 31)
            planes.append((words & jnp.int32(mask)).astype(jnp.float32).astype(jnp.bfloat16))
        return jnp.concatenate(planes, axis=0)

    for first in range(0, cols, chunk):
        part = slice(first, first + chunk)
        term = jnp.dot(z1_ref[...], edges(b13_ref[0, :, part]), preferred_element_type=jnp.float32)
        acc[:, part] = term + jnp.dot(
            z2_ref[...], edges(b2_ref[:, part]), preferred_element_type=jnp.float32
        )
    fetch.wait()
    class_ids = lax.broadcasted_iota(jnp.int32, (padded, chunk), 0)
    summed = jnp.zeros((1, chunk), jnp.float32)
    for first in range(0, cols, chunk):
        part = slice(first, first + chunk)
        term = acc[:, part] + jnp.dot(
            z3_ref[...], edges(b13_ref[1, :, part]), preferred_element_type=jnp.float32
        )
        logits = total_ref[:, part] + term / FAN2
        powers = jnp.where(class_ids < classes, jnp.exp(logits), 0.0)
        picked = jnp.where(class_ids == label_ref[:, part], logits, 0.0)
        loss = jnp.log(jnp.sum(powers, 0, keepdims=True)) - jnp.sum(picked, 0, keepdims=True)
        loss_ref[:, part] = loss
        summed = summed + loss
    mean = jnp.sum(summed, keepdims=True) / (cols * sum_ref.shape[0])
    sum_ref[...] = jnp.broadcast_to(mean.reshape(1, 1, 1), sum_ref.shape)


def final_kernel(loss_ref, parts_ref, out_ref, mean_ref):
    out_ref[...] = loss_ref[...]
    mean_ref[0, 0] = jnp.sum(parts_ref[:, :, 0:1])


def local(
    features,
    edges_one,
    w1_self,
    w1_nbr,
    need_blocks,
    live_slots,
    edges_two,
    w2_self,
    w2_nbr,
    labels,
):
    rows, block_len = features.shape
    hid = w1_self.shape[1]
    depth, classes = w2_self.shape
    nodes = lax.axis_size("node")
    feats = lax.axis_size("feat")
    height = pl.cdiv(rows, 8) * 8
    width = block_len + 2 * hid + depth // height * LANES
    padded = pl.cdiv(classes, 16) * 16

    packed, early = pl.pallas_call(
        pack_kernel,
        out_shape=(
            jax.ShapeDtypeStruct((height, width), jnp.bfloat16),
            jax.ShapeDtypeStruct((block_len // 2, block_len), jnp.int32),
        ),
        in_specs=[HBM] * 6,
        out_specs=(VMEM, VMEM),
        scratch_shapes=[
            pltpu.VMEM((rows, block_len), jnp.bfloat16),
            pltpu.VMEM((rows, hid), jnp.bfloat16),
            pltpu.VMEM((rows, hid), jnp.bfloat16),
            pltpu.VMEM((classes, depth), jnp.bfloat16),
            pltpu.VMEM((classes, depth), jnp.bfloat16),
            pltpu.VMEM((height, block_len + 2 * hid), jnp.float32),
            pltpu.VMEM((LANES, LANES), jnp.float32),
            pltpu.SemaphoreType.DMA((6,)),
        ],
        compiler_params=pltpu.CompilerParams(vmem_limit_bytes=4 * MIB),
        cost_estimate=pl.CostEstimate(flops=2 * MIB, bytes_accessed=2 * MIB, transcendentals=0),
        name="pack",
    )(*map(in_hbm, (features, w1_self, w1_nbr, w2_self.T, w2_nbr.T, edges_one)))

    blocks = [packed] + [from_ahead(packed, "feat", step) for step in (2, 3, 1)]
    words = block_len // 32
    adjacency, bits_outer, number = pl.pallas_call(
        functools.partial(load_kernel, nodes),
        out_shape=(
            jax.ShapeDtypeStruct(edges_one.shape, jnp.bfloat16),
            jax.ShapeDtypeStruct((2, words, block_len), jnp.int32),
            jax.ShapeDtypeStruct((1,), jnp.int32),
        ),
        in_specs=[HBM, VMEM, HBM, HBM, HBM],
        out_specs=(VMEM, VMEM, SMEM),
        scratch_shapes=[
            pltpu.SMEM(need_blocks.shape, jnp.int32),
            pltpu.SMEM(live_slots.shape, jnp.int32),
            pltpu.VMEM((10, block_len // 4, block_len), jnp.int32),
            pltpu.SemaphoreType.DMA((12,)),
        ],
        compiler_params=pltpu.CompilerParams(vmem_limit_bytes=16 * MIB),
        cost_estimate=pl.CostEstimate(flops=100 * MIB, bytes_accessed=10 * MIB, transcendentals=0),
        name="load",
    )(in_hbm(edges_one), early, *map(in_hbm, (edges_two, need_blocks, live_slots)))
    taken = (0, nodes // 2, nodes - 1)
    steps = [step for step in range(nodes) if step not in taken]
    number = lax.clamp(0, number[0], len(steps) - 1)

    self_term, mine, send, own = pl.pallas_call(
        functools.partial(first_kernel, hid, depth),
        out_shape=(
            jax.ShapeDtypeStruct((padded, block_len), jnp.float32),
            jax.ShapeDtypeStruct((padded, block_len), jnp.bfloat16),
            jax.ShapeDtypeStruct((padded, block_len), jnp.bfloat16),
            jax.ShapeDtypeStruct((padded, block_len), jnp.bfloat16),
        ),
        in_specs=[VMEM] * 5 + [HBM],
        out_specs=(VMEM,) * 4,
        scratch_shapes=[
            pltpu.VMEM((feats * height, block_len), jnp.bfloat16),
            pltpu.VMEM((2 * feats * height, hid), jnp.bfloat16),
            pltpu.VMEM((feats * depth, LANES), jnp.bfloat16),
        ],
        compiler_params=pltpu.CompilerParams(vmem_limit_bytes=16 * MIB),
        cost_estimate=pl.CostEstimate(
            flops=2 * 128 * block_len * block_len, bytes_accessed=4 * MIB, transcendentals=0
        ),
        name="first",
    )(*blocks, adjacency, in_hbm(number[None]))

    behind = from_ahead(mine, "node", nodes - 1)
    half = from_ahead(mine, "node", nodes // 2)

    def with_offset(step, send, own, self_term, edges_two, live_slots):
        fourth = from_ahead(send, "node", step)
        total, bits_two = pl.pallas_call(
            stream_kernel,
            out_shape=(
                jax.ShapeDtypeStruct((padded, block_len), jnp.float32),
                jax.ShapeDtypeStruct((words, block_len), jnp.int32),
            ),
            in_specs=[VMEM, VMEM, HBM, HBM],
            out_specs=(VMEM, VMEM),
            scratch_shapes=[
                pltpu.VMEM((8, block_len // 4, block_len), jnp.int32),
                pltpu.VMEM((padded, block_len), jnp.float32),
                pltpu.SMEM(live_slots.shape, jnp.int32),
                pltpu.SemaphoreType.DMA((9,)),
            ],
            compiler_params=pltpu.CompilerParams(vmem_limit_bytes=12 * MIB),
            cost_estimate=pl.CostEstimate(
                flops=100 * MIB, bytes_accessed=8 * MIB, transcendentals=0
            ),
            name="stream",
        )(own, self_term, in_hbm(edges_two), in_hbm(live_slots))
        return fourth, total, bits_two

    fourth, total, bits_two = lax.switch(
        number,
        [functools.partial(with_offset, step) for step in steps],
        send,
        own,
        self_term,
        edges_two,
        live_slots,
    )

    loss, sums = pl.pallas_call(
        functools.partial(second_kernel, classes),
        out_shape=(
            jax.ShapeDtypeStruct((1, block_len), jnp.float32),
            jax.ShapeDtypeStruct((nodes, 1, LANES), jnp.float32),
        ),
        in_specs=[VMEM, VMEM, HBM] + [VMEM] * 4,
        out_specs=(VMEM, VMEM),
        scratch_shapes=[
            pltpu.VMEM((padded, block_len), jnp.bfloat16),
            pltpu.VMEM((padded, block_len), jnp.float32),
            pltpu.SemaphoreType.DMA,
        ],
        compiler_params=pltpu.CompilerParams(vmem_limit_bytes=16 * MIB),
        cost_estimate=pl.CostEstimate(
            flops=2 * 64 * 3 * block_len * block_len,
            bytes_accessed=2 * MIB,
            transcendentals=padded * block_len,
        ),
        name="second",
    )(behind, half, in_hbm(fourth), total, bits_outer, bits_two, labels[None, :])

    everyone = lax.all_to_all(sums, "node", 0, 0, tiled=True)
    node_loss, mean_loss = pl.pallas_call(
        final_kernel,
        out_shape=(
            jax.ShapeDtypeStruct((1, block_len), jnp.float32),
            jax.ShapeDtypeStruct((1, 1), jnp.float32),
        ),
        in_specs=[VMEM, VMEM],
        out_specs=(VMEM, SMEM),
        compiler_params=pltpu.CompilerParams(vmem_limit_bytes=1 * MIB),
        name="final",
    )(loss, everyone)
    return (node_loss[0], mean_loss[0, 0])


def solution(mesh):
    return jax.shard_map(
        local,
        mesh=mesh,
        in_specs=(
            P("feat", "node"),
            P(None, "node"),
            P("feat", None),
            P("feat", None),
            P("node", None),
            P("node", None),
            P(None, "node"),
            P("feat", None),
            P("feat", None),
            P("node"),
        ),
        out_specs=(P("node"), P()),
        check_vma=False,
    )
```

```python
import functools

import jax
import jax.numpy as jnp
from jax import lax
from jax.experimental import pallas as pl
from jax.experimental.pallas import tpu as pltpu
from jax.sharding import PartitionSpec as P

FAN1 = 25
FAN2 = 10
LANES = 128
WORDS = 32
EARLY = 2
MIB = 1 << 20

VMEM = pl.BlockSpec(memory_space=pltpu.VMEM)
HBM = pl.BlockSpec(memory_space=pltpu.HBM)
SMEM = pl.BlockSpec(memory_space=pltpu.SMEM)


def in_hbm(value):
    return pltpu.with_memory_space_constraint(value, pltpu.HBM)


def from_ahead(value, axis, steps):
    count = lax.axis_size(axis)
    pairs = [(source, (source - steps) % count) for source in range(count)]
    return lax.ppermute(value, axis, pairs)


def pack_kernel(*refs):
    sources, out_ref, held, (scr, cat, sems) = refs[:5], refs[5], refs[6:11], refs[11:]
    copies = [
        pltpu.make_async_copy(source, place, sems.at[index])
        for index, (source, place) in enumerate(zip(sources, held))
    ]
    for copy in copies:
        copy.start()
    x_ref, ws_ref, wn_ref, us_ref, un_ref = held
    rows, cols = x_ref.shape
    hid = ws_ref.shape[1]
    classes, depth = us_ref.shape
    height = out_ref.shape[0]
    side = cols + 2 * hid
    scr[rows:, :] = jnp.zeros((height - rows, side), jnp.float32)
    cat[...] = jnp.zeros_like(cat)
    for copy in copies:
        copy.wait()
    scr[:rows, :cols] = x_ref[...].astype(jnp.float32)
    scr[:rows, cols : cols + hid] = ws_ref[...].astype(jnp.float32)
    scr[:rows, cols + hid :] = wn_ref[...].astype(jnp.float32)
    cat[:classes, :depth] = us_ref[...].astype(jnp.float32)
    cat[LANES // 2 : LANES // 2 + classes, :depth] = un_ref[...].astype(jnp.float32)
    by_unit = cat[...].T
    out_ref[:, :side] = scr[...].astype(jnp.bfloat16)
    for piece in range(depth // height):
        place = slice(side + piece * LANES, side + (piece + 1) * LANES)
        out_ref[:, place] = by_unit[piece * height : (piece + 1) * height].astype(jnp.bfloat16)


def packed_bits(piece, first_bit):
    words = None
    for group in range(piece.shape[0] // WORDS):
        bits = piece[group * WORDS : (group + 1) * WORDS, :] << (first_bit + group)
        words = bits if words is None else words | bits
    return words


def pack_slot(pieces, first_bit):
    words = None
    for index, arrived in enumerate(pieces):
        piece = arrived()
        bits = packed_bits(piece, first_bit + index * (piece.shape[0] // WORDS))
        words = bits if words is None else words | bits
    return words


def load_kernel(
    nodes, e1_ref, e2_ref, need_ref, live_ref, after_ref, e1_out, bits_ref, number_ref, need, live, held, sems
):
    rows = held.shape[1]
    cols = e1_out.shape[0]
    per_slot = cols // rows
    extra = held.shape[0] - 2 * per_slot
    sources = [e1_ref.at[pl.ds(index * rows, rows)] for index in range(per_slot)]
    sources += [e2_ref.at[pl.ds(cols + index * rows, rows)] for index in range(per_slot)]
    sources += [e2_ref.at[pl.ds(3 * cols + index * rows, rows)] for index in range(extra)]
    copies = [
        pltpu.make_async_copy(source, held.at[index], sems.at[index])
        for index, source in enumerate(sources)
    ]
    small = [
        pltpu.make_async_copy(need_ref, need, sems.at[len(sources)]),
        pltpu.make_async_copy(live_ref, live, sems.at[len(sources) + 1]),
    ]
    for copy in small + copies:
        copy.start()
    for copy in small:
        copy.wait()
    offset = lax.rem(need[0, 3] - lax.axis_index("node") + nodes, nodes)
    number_ref[0] = offset - 1 - (offset > nodes // 2).astype(jnp.int32)

    def arrived(index):
        copies[index].wait()
        return held.at[index]

    for index in range(per_slot):
        piece = arrived(index)[...].astype(jnp.float32).astype(jnp.bfloat16)
        e1_out[index * rows : (index + 1) * rows, :] = piece
    for place, slot, begin, count in ((0, 1, per_slot, per_slot), (1, 3, 2 * per_slot, extra)):
        pieces = [functools.partial(arrived, begin + index) for index in range(count)]
        bits_ref[place] = jnp.where(live[0, slot] == 1, pack_slot(pieces, 0), 0)


def stream_kernel(z_ref, self_ref, e2_ref, live_ref, total_ref, bits_ref, held, acc, live, sems):
    rows = held.shape[1]
    cols = z_ref.shape[1]
    pieces = cols // rows
    late = held.shape[0] - 2 * pieces
    sources = [slot * pieces + index for slot in (0, 2) for index in range(pieces)]
    sources += [4 * pieces - late + index for index in range(late)]
    copies = [
        pltpu.make_async_copy(e2_ref.at[pl.ds(source * rows, rows)], held.at[index], sems.at[index])
        for index, source in enumerate(sources)
    ]
    copies.append(pltpu.make_async_copy(live_ref, live, sems.at[len(sources)]))
    for copy in copies:
        copy.start()
    acc[...] = jnp.zeros_like(acc)

    def arrived(index):
        pltpu.make_async_copy(e2_ref.at[pl.ds(0, rows)], held.at[index], sems.at[index]).wait()
        return held.at[index]

    @pl.loop(0, pieces)
    def _(index):
        adjacency = arrived(index)[...].astype(jnp.float32).astype(jnp.bfloat16)
        own = z_ref[:, pl.ds(pl.multiple_of(index * rows, rows), rows)]
        acc[...] += jnp.dot(own, adjacency, preferred_element_type=jnp.float32)

    total_ref[...] = self_ref[...] + acc[...] / FAN2
    bits_ref[...] = jnp.zeros_like(bits_ref)

    for place, begin, count in ((0, pieces, pieces), (1, 2 * pieces, late)):

        @pl.loop(0, count)
        def _(index):
            first_bit = (index + pieces - count) * (rows // WORDS)
            bits_ref[place] = bits_ref[place] | packed_bits(arrived(begin + index), first_bit)

    copies[-1].wait()
    for place, slot in enumerate((2, 3)):
        bits_ref[place] = jnp.where(live[0, slot] == 1, bits_ref[place], 0)


def first_kernel(
    hid, depth, p0_ref, p2_ref, p3_ref, p1_ref, e_ref, after_ref, self_ref, z_ref, send_ref, own_ref, x, w1, w2
):
    me = lax.axis_index("feat")
    height = p0_ref.shape[0]
    cols = x.shape[1]
    feats = x.shape[0] // height
    padded = z_ref.shape[0]
    for step, ref in enumerate((p0_ref, p1_ref, p2_ref, p3_ref)):
        place = lax.rem(me + step, feats)
        rows = pl.ds(pl.multiple_of(place * height, height), height)
        x[rows, :] = ref[:, :cols]
        w1[rows, :] = ref[:, cols : cols + hid]
        below = pl.ds(pl.multiple_of((feats + place) * height, height), height)
        w1[below, :] = ref[:, cols + hid : cols + 2 * hid]
        for piece in range(depth // height):
            units = pl.ds(pl.multiple_of(place * depth + piece * height, height), height)
            lanes = slice(cols + 2 * hid + piece * LANES, cols + 2 * hid + (piece + 1) * LANES)
            w2[units, :] = ref[:, lanes]
    inputs = x[...]
    weights = w1[...].astype(jnp.float32).T.astype(jnp.bfloat16)
    project = w2[...].astype(jnp.float32).T.astype(jnp.bfloat16)
    group = lax.broadcasted_iota(jnp.int32, (1, cols), 1) // WORDS
    scale = jnp.ones((1, cols), jnp.float32)
    for bit in range(5):
        scale = scale * jnp.where((group >> bit) % 2 == 1, 2.0 ** -(1 << bit), 1.0)
    scale = jnp.where(group == 31, -scale, scale)
    nbr = jnp.dot(inputs, e_ref[...], preferred_element_type=jnp.float32) / FAN1
    stacked = jnp.concatenate([inputs, nbr.astype(jnp.bfloat16)], axis=0)
    before = jnp.dot(weights, stacked, preferred_element_type=jnp.float32)
    hidden = jnp.maximum(before, 0.0).astype(jnp.bfloat16)
    both = jnp.dot(project, hidden, preferred_element_type=jnp.float32)
    self_ref[...] = both[:padded]
    z = both[LANES // 2 : LANES // 2 + padded]
    own_ref[...] = z.astype(jnp.bfloat16)
    scaled = (z * scale).astype(jnp.bfloat16)
    z_ref[...] = scaled
    send_ref[...] = scaled


def second_kernel(
    classes, z2_ref, z1_ref, z3_hbm, total_ref, b13_ref, b23_ref, label_ref, loss_ref, sum_ref, z3_ref, acc, sem
):
    padded, cols = total_ref.shape
    fetch = pltpu.make_async_copy(z3_hbm, z3_ref, sem)
    fetch.start()
    chunk = 256

    def edges(words):
        planes = []
        for bit in range(32):
            mask = (1 << bit) if bit < 31 else -(1 << 31)
            planes.append((words & jnp.int32(mask)).astype(jnp.float32).astype(jnp.bfloat16))
        return jnp.concatenate(planes, axis=0)

    for first in range(0, cols, chunk):
        part = slice(first, first + chunk)
        term = jnp.dot(z1_ref[...], edges(b13_ref[0, :, part]), preferred_element_type=jnp.float32)
        acc[:, part] = term + jnp.dot(
            z2_ref[...], edges(b23_ref[0, :, part]), preferred_element_type=jnp.float32
        )
    fetch.wait()
    class_ids = lax.broadcasted_iota(jnp.int32, (padded, chunk), 0)
    summed = jnp.zeros((1, chunk), jnp.float32)
    for first in range(0, cols, chunk):
        part = slice(first, first + chunk)
        term = acc[:, part] + jnp.dot(
            z3_ref[...],
            edges(b13_ref[1, :, part] | b23_ref[1, :, part]), preferred_element_type=jnp.float32
        )
        logits = total_ref[:, part] + term / FAN2
        powers = jnp.where(class_ids < classes, jnp.exp(logits), 0.0)
        picked = jnp.where(class_ids == label_ref[:, part], logits, 0.0)
        loss = jnp.log(jnp.sum(powers, 0, keepdims=True)) - jnp.sum(picked, 0, keepdims=True)
        loss_ref[:, part] = loss
        summed = summed + loss
    mean = jnp.sum(summed, keepdims=True) / (cols * sum_ref.shape[0])
    sum_ref[...] = jnp.broadcast_to(mean.reshape(1, 1, 1), sum_ref.shape)


def final_kernel(loss_ref, parts_ref, out_ref, mean_ref):
    out_ref[...] = loss_ref[...]
    mean_ref[0, 0] = jnp.sum(parts_ref[:, :, 0:1])


def local(
    features,
    edges_one,
    w1_self,
    w1_nbr,
    need_blocks,
    live_slots,
    edges_two,
    w2_self,
    w2_nbr,
    labels,
):
    rows, block_len = features.shape
    hid = w1_self.shape[1]
    depth, classes = w2_self.shape
    nodes = lax.axis_size("node")
    feats = lax.axis_size("feat")
    height = pl.cdiv(rows, 8) * 8
    width = block_len + 2 * hid + depth // height * LANES
    padded = pl.cdiv(classes, 16) * 16

    packed = pl.pallas_call(
        pack_kernel,
        out_shape=jax.ShapeDtypeStruct((height, width), jnp.bfloat16),
        in_specs=[HBM] * 5,
        out_specs=VMEM,
        scratch_shapes=[
            pltpu.VMEM((rows, block_len), jnp.bfloat16),
            pltpu.VMEM((rows, hid), jnp.bfloat16),
            pltpu.VMEM((rows, hid), jnp.bfloat16),
            pltpu.VMEM((classes, depth), jnp.bfloat16),
            pltpu.VMEM((classes, depth), jnp.bfloat16),
            pltpu.VMEM((height, block_len + 2 * hid), jnp.float32),
            pltpu.VMEM((LANES, LANES), jnp.float32),
            pltpu.SemaphoreType.DMA((5,)),
        ],
        compiler_params=pltpu.CompilerParams(vmem_limit_bytes=4 * MIB),
        cost_estimate=pl.CostEstimate(flops=2 * MIB, bytes_accessed=MIB // 4, transcendentals=0),
        name="pack",
    )(*map(in_hbm, (features, w1_self, w1_nbr, w2_self.T, w2_nbr.T)))

    blocks = [packed] + [from_ahead(packed, "feat", step) for step in (2, 3, 1)]
    words = block_len // 32
    adjacency, bits_outer, number = pl.pallas_call(
        functools.partial(load_kernel, nodes),
        out_shape=(
            jax.ShapeDtypeStruct(edges_one.shape, jnp.bfloat16),
            jax.ShapeDtypeStruct((2, words, block_len), jnp.int32),
            jax.ShapeDtypeStruct((1,), jnp.int32),
        ),
        in_specs=[HBM] * 4 + [VMEM],
        out_specs=(VMEM, VMEM, SMEM),
        scratch_shapes=[
            pltpu.SMEM(need_blocks.shape, jnp.int32),
            pltpu.SMEM(live_slots.shape, jnp.int32),
            pltpu.VMEM((8 + EARLY, block_len // 4, block_len), jnp.int32),
            pltpu.SemaphoreType.DMA((10 + EARLY,)),
        ],
        compiler_params=pltpu.CompilerParams(vmem_limit_bytes=16 * MIB),
        cost_estimate=pl.CostEstimate(flops=100 * MIB, bytes_accessed=10 * MIB, transcendentals=0),
        name="load",
    )(*map(in_hbm, (edges_one, edges_two, need_blocks, live_slots)), packed)
    taken = (0, nodes // 2, nodes - 1)
    steps = [step for step in range(nodes) if step not in taken]
    number = lax.clamp(0, number[0], len(steps) - 1)

    self_term, mine, send, own = pl.pallas_call(
        functools.partial(first_kernel, hid, depth),
        out_shape=(
            jax.ShapeDtypeStruct((padded, block_len), jnp.float32),
            jax.ShapeDtypeStruct((padded, block_len), jnp.bfloat16),
            jax.ShapeDtypeStruct((padded, block_len), jnp.bfloat16),
            jax.ShapeDtypeStruct((padded, block_len), jnp.bfloat16),
        ),
        in_specs=[VMEM] * 5 + [HBM],
        out_specs=(VMEM,) * 4,
        scratch_shapes=[
            pltpu.VMEM((feats * height, block_len), jnp.bfloat16),
            pltpu.VMEM((2 * feats * height, hid), jnp.bfloat16),
            pltpu.VMEM((feats * depth, LANES), jnp.bfloat16),
        ],
        compiler_params=pltpu.CompilerParams(vmem_limit_bytes=16 * MIB),
        cost_estimate=pl.CostEstimate(
            flops=2 * 128 * block_len * block_len, bytes_accessed=4 * MIB, transcendentals=0
        ),
        name="first",
    )(*blocks, adjacency, in_hbm(number[None]))

    behind = from_ahead(mine, "node", nodes - 1)
    half = from_ahead(mine, "node", nodes // 2)

    def with_offset(step, send, own, self_term, edges_two, live_slots):
        fourth = from_ahead(send, "node", step)
        total, bits_two = pl.pallas_call(
            stream_kernel,
            out_shape=(
                jax.ShapeDtypeStruct((padded, block_len), jnp.float32),
                jax.ShapeDtypeStruct((2, words, block_len), jnp.int32),
            ),
            in_specs=[VMEM, VMEM, HBM, HBM],
            out_specs=(VMEM, VMEM),
            scratch_shapes=[
                pltpu.VMEM((12 - EARLY, block_len // 4, block_len), jnp.int32),
                pltpu.VMEM((padded, block_len), jnp.float32),
                pltpu.SMEM(live_slots.shape, jnp.int32),
                pltpu.SemaphoreType.DMA((13 - EARLY,)),
            ],
            compiler_params=pltpu.CompilerParams(vmem_limit_bytes=16 * MIB),
            cost_estimate=pl.CostEstimate(
                flops=100 * MIB, bytes_accessed=8 * MIB, transcendentals=0
            ),
            name="stream",
        )(own, self_term, in_hbm(edges_two), in_hbm(live_slots))
        return fourth, total, bits_two

    fourth, total, bits_two = lax.switch(
        number,
        [functools.partial(with_offset, step) for step in steps],
        send,
        own,
        self_term,
        edges_two,
        live_slots,
    )

    loss, sums = pl.pallas_call(
        functools.partial(second_kernel, classes),
        out_shape=(
            jax.ShapeDtypeStruct((1, block_len), jnp.float32),
            jax.ShapeDtypeStruct((nodes, 1, LANES), jnp.float32),
        ),
        in_specs=[VMEM, VMEM, HBM] + [VMEM] * 4,
        out_specs=(VMEM, VMEM),
        scratch_shapes=[
            pltpu.VMEM((padded, block_len), jnp.bfloat16),
            pltpu.VMEM((padded, block_len), jnp.float32),
            pltpu.SemaphoreType.DMA,
        ],
        compiler_params=pltpu.CompilerParams(vmem_limit_bytes=16 * MIB),
        cost_estimate=pl.CostEstimate(
            flops=2 * 64 * 3 * block_len * block_len,
            bytes_accessed=2 * MIB,
            transcendentals=padded * block_len,
        ),
        name="second",
    )(behind, half, in_hbm(fourth), total, bits_outer, bits_two, labels[None, :])

    everyone = lax.all_to_all(sums, "node", 0, 0, tiled=True)
    node_loss, mean_loss = pl.pallas_call(
        final_kernel,
        out_shape=(
            jax.ShapeDtypeStruct((1, block_len), jnp.float32),
            jax.ShapeDtypeStruct((1, 1), jnp.float32),
        ),
        in_specs=[VMEM, VMEM],
        out_specs=(VMEM, SMEM),
        compiler_params=pltpu.CompilerParams(vmem_limit_bytes=1 * MIB),
        name="final",
    )(loss, everyone)
    return (node_loss[0], mean_loss[0, 0])


def solution(mesh):
    return jax.shard_map(
        local,
        mesh=mesh,
        in_specs=(
            P("feat", "node"),
            P(None, "node"),
            P("feat", None),
            P("feat", None),
            P("node", None),
            P("node", None),
            P(None, "node"),
            P("feat", None),
            P("feat", None),
            P("node"),
        ),
        out_specs=(P("node"), P()),
        check_vma=False,
    )
```

```python
import functools

import jax
import jax.numpy as jnp
from jax import lax
from jax.experimental import pallas as pl
from jax.experimental.pallas import tpu as pltpu
from jax.sharding import PartitionSpec as P

FAN1 = 25
FAN2 = 10
LANES = 128
WORDS = 32
EARLY = 1
MIB = 1 << 20

VMEM = pl.BlockSpec(memory_space=pltpu.VMEM)
HBM = pl.BlockSpec(memory_space=pltpu.HBM)
SMEM = pl.BlockSpec(memory_space=pltpu.SMEM)


def switch_in_range(number, branches, *operands):
    traced = jax.make_jaxpr(lambda index, *rest: lax.switch(index, branches, *rest))(
        number, *operands
    )
    known = dict(zip(traced.jaxpr.invars, (number, *operands)))
    known.update(zip(traced.jaxpr.constvars, traced.consts))
    (chosen,) = [each for each in traced.jaxpr.eqns if each.primitive.name == "cond"]
    values = [known[each] for each in chosen.invars[1:]]
    return chosen.primitive.bind(number, *values, **chosen.params)


def in_hbm(value):
    return pltpu.with_memory_space_constraint(value, pltpu.HBM)


def from_ahead(value, axis, steps):
    count = lax.axis_size(axis)
    pairs = [(source, (source - steps) % count) for source in range(count)]
    return lax.ppermute(value, axis, pairs)


def pack_kernel(*refs):
    sources, out_ref, held, (scr, cat, sems) = refs[:5], refs[5], refs[6:11], refs[11:]
    copies = [
        pltpu.make_async_copy(source, place, sems.at[index])
        for index, (source, place) in enumerate(zip(sources, held))
    ]
    for copy in copies:
        copy.start()
    x_ref, ws_ref, wn_ref, us_ref, un_ref = held
    rows, cols = x_ref.shape
    hid = ws_ref.shape[1]
    classes, depth = us_ref.shape
    height = out_ref.shape[0]
    side = cols + 2 * hid
    scr[rows:, :] = jnp.zeros((height - rows, side), jnp.float32)
    cat[...] = jnp.zeros_like(cat)
    for copy in copies:
        copy.wait()
    scr[:rows, :cols] = x_ref[...].astype(jnp.float32)
    scr[:rows, cols : cols + hid] = ws_ref[...].astype(jnp.float32)
    scr[:rows, cols + hid :] = wn_ref[...].astype(jnp.float32)
    cat[:classes, :depth] = us_ref[...].astype(jnp.float32)
    cat[LANES // 2 : LANES // 2 + classes, :depth] = un_ref[...].astype(jnp.float32)
    by_unit = cat[...].T
    out_ref[:, :side] = scr[...].astype(jnp.bfloat16)
    for piece in range(depth // height):
        place = slice(side + piece * LANES, side + (piece + 1) * LANES)
        out_ref[:, place] = by_unit[piece * height : (piece + 1) * height].astype(jnp.bfloat16)


def packed_bits(piece, first_bit):
    words = None
    for group in range(piece.shape[0] // WORDS):
        bits = piece[group * WORDS : (group + 1) * WORDS, :] << (first_bit + group)
        words = bits if words is None else words | bits
    return words


def pack_slot(pieces, first_bit):
    words = None
    for index, arrived in enumerate(pieces):
        piece = arrived()
        bits = packed_bits(piece, first_bit + index * (piece.shape[0] // WORDS))
        words = bits if words is None else words | bits
    return words


def load_kernel(
    nodes, e1_ref, e2_ref, need_ref, live_ref, after_ref, e1_out, bits_ref, number_ref, need, live, held, sems
):
    rows = held.shape[1]
    cols = e1_out.shape[0]
    per_slot = cols // rows
    extra = held.shape[0] - 2 * per_slot
    sources = [e1_ref.at[pl.ds(index * rows, rows)] for index in range(per_slot)]
    sources += [e2_ref.at[pl.ds(cols + index * rows, rows)] for index in range(per_slot)]
    sources += [e2_ref.at[pl.ds(3 * cols + index * rows, rows)] for index in range(extra)]
    copies = [
        pltpu.make_async_copy(source, held.at[index], sems.at[index])
        for index, source in enumerate(sources)
    ]
    small = [
        pltpu.make_async_copy(need_ref, need, sems.at[len(sources)]),
        pltpu.make_async_copy(live_ref, live, sems.at[len(sources) + 1]),
    ]
    for copy in small + copies:
        copy.start()
    for copy in small:
        copy.wait()
    offset = lax.rem(need[0, 3] - lax.axis_index("node") + nodes, nodes)
    number_ref[0] = offset - 1 - (offset > nodes // 2).astype(jnp.int32)

    def arrived(index):
        copies[index].wait()
        return held.at[index]

    for index in range(per_slot):
        piece = arrived(index)[...].astype(jnp.float32).astype(jnp.bfloat16)
        e1_out[index * rows : (index + 1) * rows, :] = piece
    for place, slot, begin, count in ((0, 1, per_slot, per_slot), (1, 3, 2 * per_slot, extra)):
        pieces = [functools.partial(arrived, begin + index) for index in range(count)]
        bits_ref[place] = jnp.where(live[0, slot] == 1, pack_slot(pieces, 0), 0)


def stream_kernel(z_ref, self_ref, e2_ref, live_ref, total_ref, bits_ref, held, acc, live, sems):
    rows = held.shape[1]
    cols = z_ref.shape[1]
    pieces = cols // rows
    late = held.shape[0] - 2 * pieces
    sources = [slot * pieces + index for slot in (0, 2) for index in range(pieces)]
    sources += [4 * pieces - late + index for index in range(late)]
    copies = [
        pltpu.make_async_copy(e2_ref.at[pl.ds(source * rows, rows)], held.at[index], sems.at[index])
        for index, source in enumerate(sources)
    ]
    copies.append(pltpu.make_async_copy(live_ref, live, sems.at[len(sources)]))
    for copy in copies:
        copy.start()
    acc[...] = jnp.zeros_like(acc)

    def arrived(index):
        pltpu.make_async_copy(e2_ref.at[pl.ds(0, rows)], held.at[index], sems.at[index]).wait()
        return held.at[index]

    @pl.loop(0, pieces)
    def _(index):
        adjacency = arrived(index)[...].astype(jnp.float32).astype(jnp.bfloat16)
        own = z_ref[:, pl.ds(pl.multiple_of(index * rows, rows), rows)]
        acc[...] += jnp.dot(own, adjacency, preferred_element_type=jnp.float32)

    total_ref[...] = self_ref[...] + acc[...] / FAN2
    bits_ref[...] = jnp.zeros_like(bits_ref)

    for place, begin, count in ((0, pieces, pieces), (1, 2 * pieces, late)):

        @pl.loop(0, count)
        def _(index):
            first_bit = (index + pieces - count) * (rows // WORDS)
            bits_ref[place] = bits_ref[place] | packed_bits(arrived(begin + index), first_bit)

    copies[-1].wait()
    for place, slot in enumerate((2, 3)):
        bits_ref[place] = jnp.where(live[0, slot] == 1, bits_ref[place], 0)


def first_kernel(
    hid, depth, p0_ref, p2_ref, p3_ref, p1_ref, e_ref, self_ref, z_ref, send_ref, own_ref, x, w1, w2
):
    me = lax.axis_index("feat")
    height = p0_ref.shape[0]
    cols = x.shape[1]
    feats = x.shape[0] // height
    padded = z_ref.shape[0]
    for step, ref in enumerate((p0_ref, p1_ref, p2_ref, p3_ref)):
        place = lax.rem(me + step, feats)
        rows = pl.ds(pl.multiple_of(place * height, height), height)
        x[rows, :] = ref[:, :cols]
        w1[rows, :] = ref[:, cols : cols + hid]
        below = pl.ds(pl.multiple_of((feats + place) * height, height), height)
        w1[below, :] = ref[:, cols + hid : cols + 2 * hid]
        for piece in range(depth // height):
            units = pl.ds(pl.multiple_of(place * depth + piece * height, height), height)
            lanes = slice(cols + 2 * hid + piece * LANES, cols + 2 * hid + (piece + 1) * LANES)
            w2[units, :] = ref[:, lanes]
    inputs = x[...]
    weights = w1[...].astype(jnp.float32).T.astype(jnp.bfloat16)
    project = w2[...].astype(jnp.float32).T.astype(jnp.bfloat16)
    group = lax.broadcasted_iota(jnp.int32, (1, cols), 1) // WORDS
    scale = jnp.ones((1, cols), jnp.float32)
    for bit in range(5):
        scale = scale * jnp.where((group >> bit) % 2 == 1, 2.0 ** -(1 << bit), 1.0)
    scale = jnp.where(group == 31, -scale, scale)
    nbr = jnp.dot(inputs, e_ref[...], preferred_element_type=jnp.float32) / FAN1
    stacked = jnp.concatenate([inputs, nbr.astype(jnp.bfloat16)], axis=0)
    before = jnp.dot(weights, stacked, preferred_element_type=jnp.float32)
    hidden = jnp.maximum(before, 0.0).astype(jnp.bfloat16)
    both = jnp.dot(project, hidden, preferred_element_type=jnp.float32)
    self_ref[...] = both[:padded]
    z = both[LANES // 2 : LANES // 2 + padded]
    own_ref[...] = z.astype(jnp.bfloat16)
    scaled = (z * scale).astype(jnp.bfloat16)
    z_ref[...] = scaled
    send_ref[...] = scaled


def second_kernel(
    classes, z2_ref, z1_ref, z3_hbm, total_ref, b13_ref, b23_ref, label_ref, loss_ref, sum_ref, z3_ref, acc, sem
):
    padded, cols = total_ref.shape
    fetch = pltpu.make_async_copy(z3_hbm, z3_ref, sem)
    fetch.start()
    chunk = 256

    def edges(words):
        planes = []
        for bit in range(32):
            mask = (1 << bit) if bit < 31 else -(1 << 31)
            planes.append((words & jnp.int32(mask)).astype(jnp.float32).astype(jnp.bfloat16))
        return jnp.concatenate(planes, axis=0)

    for first in range(0, cols, chunk):
        part = slice(first, first + chunk)
        term = jnp.dot(z1_ref[...], edges(b13_ref[0, :, part]), preferred_element_type=jnp.float32)
        acc[:, part] = term + jnp.dot(
            z2_ref[...], edges(b23_ref[0, :, part]), preferred_element_type=jnp.float32
        )
    fetch.wait()
    class_ids = lax.broadcasted_iota(jnp.int32, (padded, chunk), 0)
    summed = jnp.zeros((1, chunk), jnp.float32)
    for first in range(0, cols, chunk):
        part = slice(first, first + chunk)
        term = acc[:, part] + jnp.dot(
            z3_ref[...],
            edges(b13_ref[1, :, part] | b23_ref[1, :, part]), preferred_element_type=jnp.float32
        )
        logits = total_ref[:, part] + term / FAN2
        powers = jnp.where(class_ids < classes, jnp.exp(logits), 0.0)
        picked = jnp.where(class_ids == label_ref[:, part], logits, 0.0)
        loss = jnp.log(jnp.sum(powers, 0, keepdims=True)) - jnp.sum(picked, 0, keepdims=True)
        loss_ref[:, part] = loss
        summed = summed + loss
    mean = jnp.sum(summed, keepdims=True) / (cols * sum_ref.shape[0])
    sum_ref[...] = jnp.broadcast_to(mean.reshape(1, 1, 1), sum_ref.shape)


def final_kernel(loss_ref, parts_ref, out_ref, mean_ref):
    out_ref[...] = loss_ref[...]
    mean_ref[0, 0] = jnp.sum(parts_ref[:, :, 0:1])


def local(
    features,
    edges_one,
    w1_self,
    w1_nbr,
    need_blocks,
    live_slots,
    edges_two,
    w2_self,
    w2_nbr,
    labels,
):
    rows, block_len = features.shape
    hid = w1_self.shape[1]
    depth, classes = w2_self.shape
    nodes = lax.axis_size("node")
    feats = lax.axis_size("feat")
    height = pl.cdiv(rows, 8) * 8
    width = block_len + 2 * hid + depth // height * LANES
    padded = pl.cdiv(classes, 16) * 16

    packed = pl.pallas_call(
        pack_kernel,
        out_shape=jax.ShapeDtypeStruct((height, width), jnp.bfloat16),
        in_specs=[HBM] * 5,
        out_specs=VMEM,
        scratch_shapes=[
            pltpu.VMEM((rows, block_len), jnp.bfloat16),
            pltpu.VMEM((rows, hid), jnp.bfloat16),
            pltpu.VMEM((rows, hid), jnp.bfloat16),
            pltpu.VMEM((classes, depth), jnp.bfloat16),
            pltpu.VMEM((classes, depth), jnp.bfloat16),
            pltpu.VMEM((height, block_len + 2 * hid), jnp.float32),
            pltpu.VMEM((LANES, LANES), jnp.float32),
            pltpu.SemaphoreType.DMA((5,)),
        ],
        compiler_params=pltpu.CompilerParams(vmem_limit_bytes=4 * MIB),
        cost_estimate=pl.CostEstimate(flops=2 * MIB, bytes_accessed=MIB // 4, transcendentals=0),
        name="pack",
    )(*map(in_hbm, (features, w1_self, w1_nbr, w2_self.T, w2_nbr.T)))

    blocks = [packed] + [from_ahead(packed, "feat", step) for step in (2, 3, 1)]
    words = block_len // 32
    adjacency, bits_outer, number = pl.pallas_call(
        functools.partial(load_kernel, nodes),
        out_shape=(
            jax.ShapeDtypeStruct(edges_one.shape, jnp.bfloat16),
            jax.ShapeDtypeStruct((2, words, block_len), jnp.int32),
            jax.ShapeDtypeStruct((1,), jnp.int32),
        ),
        in_specs=[HBM] * 4 + [VMEM],
        out_specs=(VMEM, VMEM, SMEM),
        scratch_shapes=[
            pltpu.SMEM(need_blocks.shape, jnp.int32),
            pltpu.SMEM(live_slots.shape, jnp.int32),
            pltpu.VMEM((8 + EARLY, block_len // 4, block_len), jnp.int32),
            pltpu.SemaphoreType.DMA((10 + EARLY,)),
        ],
        compiler_params=pltpu.CompilerParams(vmem_limit_bytes=16 * MIB),
        cost_estimate=pl.CostEstimate(flops=100 * MIB, bytes_accessed=10 * MIB, transcendentals=0),
        name="load",
    )(*map(in_hbm, (edges_one, edges_two, need_blocks, live_slots)), packed)
    taken = (0, nodes // 2, nodes - 1)
    steps = [step for step in range(nodes) if step not in taken]

    self_term, mine, send, own = pl.pallas_call(
        functools.partial(first_kernel, hid, depth),
        out_shape=(
            jax.ShapeDtypeStruct((padded, block_len), jnp.float32),
            jax.ShapeDtypeStruct((padded, block_len), jnp.bfloat16),
            jax.ShapeDtypeStruct((padded, block_len), jnp.bfloat16),
            jax.ShapeDtypeStruct((padded, block_len), jnp.bfloat16),
        ),
        in_specs=[VMEM] * 5,
        out_specs=(VMEM,) * 4,
        scratch_shapes=[
            pltpu.VMEM((feats * height, block_len), jnp.bfloat16),
            pltpu.VMEM((2 * feats * height, hid), jnp.bfloat16),
            pltpu.VMEM((feats * depth, LANES), jnp.bfloat16),
        ],
        compiler_params=pltpu.CompilerParams(vmem_limit_bytes=16 * MIB),
        cost_estimate=pl.CostEstimate(
            flops=2 * 128 * block_len * block_len, bytes_accessed=4 * MIB, transcendentals=0
        ),
        name="first",
    )(*blocks, adjacency)

    behind = from_ahead(mine, "node", nodes - 1)
    half = from_ahead(mine, "node", nodes // 2)

    def with_offset(step, send, own, self_term, edges_two, live_slots):
        fourth = from_ahead(send, "node", step)
        total, bits_two = pl.pallas_call(
            stream_kernel,
            out_shape=(
                jax.ShapeDtypeStruct((padded, block_len), jnp.float32),
                jax.ShapeDtypeStruct((2, words, block_len), jnp.int32),
            ),
            in_specs=[VMEM, VMEM, HBM, HBM],
            out_specs=(VMEM, VMEM),
            scratch_shapes=[
                pltpu.VMEM((12 - EARLY, block_len // 4, block_len), jnp.int32),
                pltpu.VMEM((padded, block_len), jnp.float32),
                pltpu.SMEM(live_slots.shape, jnp.int32),
                pltpu.SemaphoreType.DMA((13 - EARLY,)),
            ],
            compiler_params=pltpu.CompilerParams(vmem_limit_bytes=16 * MIB),
            cost_estimate=pl.CostEstimate(
                flops=100 * MIB, bytes_accessed=8 * MIB, transcendentals=0
            ),
            name="stream",
        )(own, self_term, in_hbm(edges_two), in_hbm(live_slots))
        return fourth, total, bits_two

    fourth, total, bits_two = switch_in_range(
        number[0],
        [functools.partial(with_offset, step) for step in steps],
        send,
        own,
        self_term,
        edges_two,
        live_slots,
    )

    loss, sums = pl.pallas_call(
        functools.partial(second_kernel, classes),
        out_shape=(
            jax.ShapeDtypeStruct((1, block_len), jnp.float32),
            jax.ShapeDtypeStruct((nodes, 1, LANES), jnp.float32),
        ),
        in_specs=[VMEM, VMEM, HBM] + [VMEM] * 4,
        out_specs=(VMEM, VMEM),
        scratch_shapes=[
            pltpu.VMEM((padded, block_len), jnp.bfloat16),
            pltpu.VMEM((padded, block_len), jnp.float32),
            pltpu.SemaphoreType.DMA,
        ],
        compiler_params=pltpu.CompilerParams(vmem_limit_bytes=16 * MIB),
        cost_estimate=pl.CostEstimate(
            flops=2 * 64 * 3 * block_len * block_len,
            bytes_accessed=2 * MIB,
            transcendentals=padded * block_len,
        ),
        name="second",
    )(behind, half, in_hbm(fourth), total, bits_outer, bits_two, labels[None, :])

    everyone = lax.all_to_all(sums, "node", 0, 0, tiled=True)
    node_loss, mean_loss = pl.pallas_call(
        final_kernel,
        out_shape=(
            jax.ShapeDtypeStruct((1, block_len), jnp.float32),
            jax.ShapeDtypeStruct((1, 1), jnp.float32),
        ),
        in_specs=[VMEM, VMEM],
        out_specs=(VMEM, SMEM),
        compiler_params=pltpu.CompilerParams(vmem_limit_bytes=1 * MIB),
        name="final",
    )(loss, everyone)
    return (node_loss[0], mean_loss[0, 0])


def solution(mesh):
    return jax.shard_map(
        local,
        mesh=mesh,
        in_specs=(
            P("feat", "node"),
            P(None, "node"),
            P("feat", None),
            P("feat", None),
            P("node", None),
            P("node", None),
            P(None, "node"),
            P("feat", None),
            P("feat", None),
            P("node"),
        ),
        out_specs=(P("node"), P()),
        check_vma=False,
    )
```

```python
import functools

import jax
import jax.numpy as jnp
from jax import lax
from jax.experimental import pallas as pl
from jax.experimental.pallas import tpu as pltpu
from jax.sharding import PartitionSpec as P

FAN1 = 25
FAN2 = 10
LANES = 128
WORDS = 32
EARLY = 2
MIB = 1 << 20

VMEM = pl.BlockSpec(memory_space=pltpu.VMEM)
HBM = pl.BlockSpec(memory_space=pltpu.HBM)
SMEM = pl.BlockSpec(memory_space=pltpu.SMEM)


def in_hbm(value):
    return pltpu.with_memory_space_constraint(value, pltpu.HBM)


def from_ahead(value, axis, steps):
    count = lax.axis_size(axis)
    pairs = [(source, (source - steps) % count) for source in range(count)]
    return lax.ppermute(value, axis, pairs)


def pack_kernel(*refs):
    sources, out_ref, held, (scr, cat, sems) = refs[:5], refs[5], refs[6:11], refs[11:]
    copies = [
        pltpu.make_async_copy(source, place, sems.at[index])
        for index, (source, place) in enumerate(zip(sources, held))
    ]
    for copy in copies:
        copy.start()
    x_ref, ws_ref, wn_ref, us_ref, un_ref = held
    rows, cols = x_ref.shape
    hid = ws_ref.shape[1]
    classes, depth = us_ref.shape
    height = out_ref.shape[0]
    side = cols + 2 * hid
    scr[rows:, :] = jnp.zeros((height - rows, side), jnp.float32)
    cat[...] = jnp.zeros_like(cat)
    for copy in copies:
        copy.wait()
    scr[:rows, :cols] = x_ref[...].astype(jnp.float32)
    scr[:rows, cols : cols + hid] = ws_ref[...].astype(jnp.float32)
    scr[:rows, cols + hid :] = wn_ref[...].astype(jnp.float32)
    cat[:classes, :depth] = us_ref[...].astype(jnp.float32)
    cat[LANES // 2 : LANES // 2 + classes, :depth] = un_ref[...].astype(jnp.float32)
    by_unit = cat[...].T
    out_ref[:, :side] = scr[...].astype(jnp.bfloat16)
    for piece in range(depth // height):
        place = slice(side + piece * LANES, side + (piece + 1) * LANES)
        out_ref[:, place] = by_unit[piece * height : (piece + 1) * height].astype(jnp.bfloat16)


def packed_bits(piece, first_bit):
    words = None
    for group in range(piece.shape[0] // WORDS):
        bits = piece[group * WORDS : (group + 1) * WORDS, :] << (first_bit + group)
        words = bits if words is None else words | bits
    return words


def pack_slot(pieces, first_bit):
    words = None
    for index, arrived in enumerate(pieces):
        piece = arrived()
        bits = packed_bits(piece, first_bit + index * (piece.shape[0] // WORDS))
        words = bits if words is None else words | bits
    return words


def load_kernel(
    nodes, e1_ref, e2_ref, need_ref, live_ref, after_ref, e1_out, bits_ref, number_ref, need, live, number, held, sems
):
    rows = held.shape[1]
    cols = e1_out.shape[0]
    per_slot = cols // rows
    extra = held.shape[0] - 2 * per_slot
    sources = [e1_ref.at[pl.ds(index * rows, rows)] for index in range(per_slot)]
    sources += [e2_ref.at[pl.ds(cols + index * rows, rows)] for index in range(per_slot)]
    sources += [e2_ref.at[pl.ds(3 * cols + index * rows, rows)] for index in range(extra)]
    copies = [
        pltpu.make_async_copy(source, held.at[index], sems.at[index])
        for index, source in enumerate(sources)
    ]
    small = [
        pltpu.make_async_copy(need_ref, need, sems.at[len(sources)]),
        pltpu.make_async_copy(live_ref, live, sems.at[len(sources) + 1]),
    ]
    for copy in small + copies:
        copy.start()
    for copy in small:
        copy.wait()
    offset = lax.rem(need[0, 3] - lax.axis_index("node") + nodes, nodes)
    number[0] = offset - 1 - (offset > nodes // 2).astype(jnp.int32)
    told = pltpu.make_async_copy(number, number_ref, sems.at[len(sources) + 2])
    told.start()

    def arrived(index):
        copies[index].wait()
        return held.at[index]

    for index in range(per_slot):
        piece = arrived(index)[...].astype(jnp.float32).astype(jnp.bfloat16)
        e1_out[index * rows : (index + 1) * rows, :] = piece
    for place, slot, begin, count in ((0, 1, per_slot, per_slot), (1, 3, 2 * per_slot, extra)):
        pieces = [functools.partial(arrived, begin + index) for index in range(count)]
        bits_ref[place] = jnp.where(live[0, slot] == 1, pack_slot(pieces, 0), 0)
    told.wait()


def stream_kernel(z_ref, self_ref, e2_ref, live_ref, total_ref, bits_ref, held, acc, live, sems):
    rows = held.shape[1]
    cols = z_ref.shape[1]
    pieces = cols // rows
    late = held.shape[0] - 2 * pieces
    sources = [slot * pieces + index for slot in (0, 2) for index in range(pieces)]
    sources += [4 * pieces - late + index for index in range(late)]
    copies = [
        pltpu.make_async_copy(e2_ref.at[pl.ds(source * rows, rows)], held.at[index], sems.at[index])
        for index, source in enumerate(sources)
    ]
    copies.append(pltpu.make_async_copy(live_ref, live, sems.at[len(sources)]))
    for copy in copies:
        copy.start()
    acc[...] = jnp.zeros_like(acc)

    def arrived(index):
        pltpu.make_async_copy(e2_ref.at[pl.ds(0, rows)], held.at[index], sems.at[index]).wait()
        return held.at[index]

    @pl.loop(0, pieces)
    def _(index):
        adjacency = arrived(index)[...].astype(jnp.float32).astype(jnp.bfloat16)
        own = z_ref[:, pl.ds(pl.multiple_of(index * rows, rows), rows)]
        acc[...] += jnp.dot(own, adjacency, preferred_element_type=jnp.float32)

    total_ref[...] = self_ref[...] + acc[...] / FAN2
    bits_ref[...] = jnp.zeros_like(bits_ref)

    for place, begin, count in ((0, pieces, pieces), (1, 2 * pieces, late)):

        @pl.loop(0, count)
        def _(index):
            first_bit = (index + pieces - count) * (rows // WORDS)
            bits_ref[place] = bits_ref[place] | packed_bits(arrived(begin + index), first_bit)

    copies[-1].wait()
    for place, slot in enumerate((2, 3)):
        bits_ref[place] = jnp.where(live[0, slot] == 1, bits_ref[place], 0)


def first_kernel(
    hid, depth, p0_ref, p2_ref, p1_ref, p3_ref, e_ref, after_ref, self_ref, z_ref, send_ref, own_ref, x, w1, w2
):
    me = lax.axis_index("feat")
    height = p0_ref.shape[0]
    cols = x.shape[1]
    feats = x.shape[0] // height
    padded = z_ref.shape[0]
    for step, ref in enumerate((p0_ref, p1_ref, p2_ref, p3_ref)):
        place = lax.rem(me + step, feats)
        rows = pl.ds(pl.multiple_of(place * height, height), height)
        x[rows, :] = ref[:, :cols]
        w1[rows, :] = ref[:, cols : cols + hid]
        below = pl.ds(pl.multiple_of((feats + place) * height, height), height)
        w1[below, :] = ref[:, cols + hid : cols + 2 * hid]
        for piece in range(depth // height):
            units = pl.ds(pl.multiple_of(place * depth + piece * height, height), height)
            lanes = slice(cols + 2 * hid + piece * LANES, cols + 2 * hid + (piece + 1) * LANES)
            w2[units, :] = ref[:, lanes]
    inputs = x[...]
    weights = w1[...].astype(jnp.float32).T.astype(jnp.bfloat16)
    project = w2[...].astype(jnp.float32).T.astype(jnp.bfloat16)
    group = lax.broadcasted_iota(jnp.int32, (1, cols), 1) // WORDS
    scale = jnp.ones((1, cols), jnp.float32)
    for bit in range(5):
        scale = scale * jnp.where((group >> bit) % 2 == 1, 2.0 ** -(1 << bit), 1.0)
    scale = jnp.where(group == 31, -scale, scale)
    nbr = jnp.dot(inputs, e_ref[...], preferred_element_type=jnp.float32) / FAN1
    stacked = jnp.concatenate([inputs, nbr.astype(jnp.bfloat16)], axis=0)
    before = jnp.dot(weights, stacked, preferred_element_type=jnp.float32)
    hidden = jnp.maximum(before, 0.0).astype(jnp.bfloat16)
    both = jnp.dot(project, hidden, preferred_element_type=jnp.float32)
    self_ref[...] = both[:padded]
    z = both[LANES // 2 : LANES // 2 + padded]
    own_ref[...] = z.astype(jnp.bfloat16)
    scaled = (z * scale).astype(jnp.bfloat16)
    z_ref[...] = scaled
    send_ref[...] = scaled


def second_kernel(
    classes, z2_ref, z1_ref, z3_ref, total_ref, b13_ref, b23_ref, label_ref, loss_ref, sum_ref, acc
):
    padded, cols = total_ref.shape
    chunk = 256

    def edges(words):
        planes = []
        for bit in range(32):
            mask = (1 << bit) if bit < 31 else -(1 << 31)
            planes.append((words & jnp.int32(mask)).astype(jnp.float32).astype(jnp.bfloat16))
        return jnp.concatenate(planes, axis=0)

    for first in range(0, cols, chunk):
        part = slice(first, first + chunk)
        term = jnp.dot(z1_ref[...], edges(b13_ref[0, :, part]), preferred_element_type=jnp.float32)
        acc[:, part] = term + jnp.dot(
            z2_ref[...], edges(b23_ref[0, :, part]), preferred_element_type=jnp.float32
        )
    class_ids = lax.broadcasted_iota(jnp.int32, (padded, chunk), 0)
    summed = jnp.zeros((1, chunk), jnp.float32)
    for first in range(0, cols, chunk):
        part = slice(first, first + chunk)
        term = acc[:, part] + jnp.dot(
            z3_ref[...],
            edges(b13_ref[1, :, part] | b23_ref[1, :, part]), preferred_element_type=jnp.float32
        )
        logits = total_ref[:, part] + term / FAN2
        powers = jnp.where(class_ids < classes, jnp.exp(logits), 0.0)
        picked = jnp.where(class_ids == label_ref[:, part], logits, 0.0)
        loss = jnp.log(jnp.sum(powers, 0, keepdims=True)) - jnp.sum(picked, 0, keepdims=True)
        loss_ref[:, part] = loss
        summed = summed + loss
    mean = jnp.sum(summed, keepdims=True) / (cols * sum_ref.shape[0])
    sum_ref[...] = jnp.broadcast_to(mean.reshape(1, 1, 1), sum_ref.shape)


def hand_on_kernel(in_ref, out_ref):
    out_ref[...] = in_ref[...]


def final_kernel(loss_ref, parts_ref, out_ref, mean_ref):
    out_ref[...] = loss_ref[...]
    mean_ref[0, 0] = jnp.sum(parts_ref[:, :, 0:1])


def local(
    features,
    edges_one,
    w1_self,
    w1_nbr,
    need_blocks,
    live_slots,
    edges_two,
    w2_self,
    w2_nbr,
    labels,
):
    rows, block_len = features.shape
    hid = w1_self.shape[1]
    depth, classes = w2_self.shape
    nodes = lax.axis_size("node")
    feats = lax.axis_size("feat")
    height = pl.cdiv(rows, 8) * 8
    width = block_len + 2 * hid + depth // height * LANES
    padded = pl.cdiv(classes, 16) * 16

    packed = pl.pallas_call(
        pack_kernel,
        out_shape=jax.ShapeDtypeStruct((height, width), jnp.bfloat16),
        in_specs=[HBM] * 5,
        out_specs=VMEM,
        scratch_shapes=[
            pltpu.VMEM((rows, block_len), jnp.bfloat16),
            pltpu.VMEM((rows, hid), jnp.bfloat16),
            pltpu.VMEM((rows, hid), jnp.bfloat16),
            pltpu.VMEM((classes, depth), jnp.bfloat16),
            pltpu.VMEM((classes, depth), jnp.bfloat16),
            pltpu.VMEM((height, block_len + 2 * hid), jnp.float32),
            pltpu.VMEM((LANES, LANES), jnp.float32),
            pltpu.SemaphoreType.DMA((5,)),
        ],
        compiler_params=pltpu.CompilerParams(vmem_limit_bytes=4 * MIB),
        cost_estimate=pl.CostEstimate(flops=2 * MIB, bytes_accessed=MIB // 4, transcendentals=0),
        name="pack",
    )(*map(in_hbm, (features, w1_self, w1_nbr, w2_self.T, w2_nbr.T)))

    blocks = [packed] + [from_ahead(packed, "feat", step) for step in (2, 1, 3)]
    words = block_len // 32
    adjacency, bits_outer, number = pl.pallas_call(
        functools.partial(load_kernel, nodes),
        out_shape=(
            jax.ShapeDtypeStruct(edges_one.shape, jnp.bfloat16),
            jax.ShapeDtypeStruct((2, words, block_len), jnp.int32),
            jax.ShapeDtypeStruct((1,), jnp.int32),
        ),
        in_specs=[HBM] * 4 + [VMEM],
        out_specs=(VMEM, VMEM, HBM),
        scratch_shapes=[
            pltpu.SMEM(need_blocks.shape, jnp.int32),
            pltpu.SMEM(live_slots.shape, jnp.int32),
            pltpu.SMEM((1,), jnp.int32),
            pltpu.VMEM((8 + EARLY, block_len // 4, block_len), jnp.int32),
            pltpu.SemaphoreType.DMA((11 + EARLY,)),
        ],
        compiler_params=pltpu.CompilerParams(vmem_limit_bytes=16 * MIB),
        cost_estimate=pl.CostEstimate(flops=100 * MIB, bytes_accessed=10 * MIB, transcendentals=0),
        name="load",
    )(*map(in_hbm, (edges_one, edges_two, need_blocks, live_slots)), packed)
    taken = (0, nodes // 2, nodes - 1)
    steps = [step for step in range(nodes) if step not in taken]
    number = lax.clamp(0, number[0], len(steps) - 1)

    self_term, mine, send, own = pl.pallas_call(
        functools.partial(first_kernel, hid, depth),
        out_shape=(
            jax.ShapeDtypeStruct((padded, block_len), jnp.float32),
            jax.ShapeDtypeStruct((padded, block_len), jnp.bfloat16),
            jax.ShapeDtypeStruct((padded, block_len), jnp.bfloat16),
            jax.ShapeDtypeStruct((padded, block_len), jnp.bfloat16),
        ),
        in_specs=[VMEM] * 5 + [HBM],
        out_specs=(VMEM,) * 4,
        scratch_shapes=[
            pltpu.VMEM((feats * height, block_len), jnp.bfloat16),
            pltpu.VMEM((2 * feats * height, hid), jnp.bfloat16),
            pltpu.VMEM((feats * depth, LANES), jnp.bfloat16),
        ],
        compiler_params=pltpu.CompilerParams(vmem_limit_bytes=16 * MIB),
        cost_estimate=pl.CostEstimate(
            flops=2 * 128 * block_len * block_len, bytes_accessed=4 * MIB, transcendentals=0
        ),
        name="first",
    )(*blocks, adjacency, in_hbm(number[None]))

    behind = from_ahead(mine, "node", nodes - 1)
    half = from_ahead(mine, "node", nodes // 2)

    def with_offset(step, send, own, self_term, edges_two, live_slots):
        fourth = from_ahead(send, "node", step)
        total, bits_two = pl.pallas_call(
            stream_kernel,
            out_shape=(
                jax.ShapeDtypeStruct((padded, block_len), jnp.float32),
                jax.ShapeDtypeStruct((2, words, block_len), jnp.int32),
            ),
            in_specs=[VMEM, VMEM, HBM, HBM],
            out_specs=(VMEM, VMEM),
            scratch_shapes=[
                pltpu.VMEM((12 - EARLY, block_len // 4, block_len), jnp.int32),
                pltpu.VMEM((padded, block_len), jnp.float32),
                pltpu.SMEM(live_slots.shape, jnp.int32),
                pltpu.SemaphoreType.DMA((13 - EARLY,)),
            ],
            compiler_params=pltpu.CompilerParams(vmem_limit_bytes=16 * MIB),
            cost_estimate=pl.CostEstimate(
                flops=100 * MIB, bytes_accessed=8 * MIB, transcendentals=0
            ),
            name="stream",
        )(own, self_term, in_hbm(edges_two), in_hbm(live_slots))
        fourth = pl.pallas_call(
            hand_on_kernel,
            out_shape=jax.ShapeDtypeStruct(fourth.shape, fourth.dtype),
            in_specs=[VMEM],
            out_specs=VMEM,
            compiler_params=pltpu.CompilerParams(vmem_limit_bytes=1 * MIB),
            name="hand_on",
        )(fourth)
        return fourth, total, bits_two

    fourth, total, bits_two = lax.switch(
        number,
        [functools.partial(with_offset, step) for step in steps],
        send,
        own,
        self_term,
        edges_two,
        live_slots,
    )

    loss, sums = pl.pallas_call(
        functools.partial(second_kernel, classes),
        out_shape=(
            jax.ShapeDtypeStruct((1, block_len), jnp.float32),
            jax.ShapeDtypeStruct((nodes, 1, LANES), jnp.float32),
        ),
        in_specs=[VMEM] * 7,
        out_specs=(VMEM, VMEM),
        scratch_shapes=[pltpu.VMEM((padded, block_len), jnp.float32)],
        compiler_params=pltpu.CompilerParams(vmem_limit_bytes=16 * MIB),
        cost_estimate=pl.CostEstimate(
            flops=2 * 64 * 3 * block_len * block_len,
            bytes_accessed=2 * MIB,
            transcendentals=padded * block_len,
        ),
        name="second",
    )(behind, half, fourth, total, bits_outer, bits_two, labels[None, :])

    everyone = lax.all_to_all(sums, "node", 0, 0, tiled=True)
    node_loss, mean_loss = pl.pallas_call(
        final_kernel,
        out_shape=(
            jax.ShapeDtypeStruct((1, block_len), jnp.float32),
            jax.ShapeDtypeStruct((1, 1), jnp.float32),
        ),
        in_specs=[VMEM, VMEM],
        out_specs=(VMEM, SMEM),
        compiler_params=pltpu.CompilerParams(vmem_limit_bytes=1 * MIB),
        name="final",
    )(loss, everyone)
    return (node_loss[0], mean_loss[0, 0])


def solution(mesh):
    return jax.shard_map(
        local,
        mesh=mesh,
        in_specs=(
            P("feat", "node"),
            P(None, "node"),
            P("feat", None),
            P("feat", None),
            P("node", None),
            P("node", None),
            P(None, "node"),
            P("feat", None),
            P("feat", None),
            P("node"),
        ),
        out_specs=(P("node"), P()),
        check_vma=False,
    )
```

```python
import functools

import jax
import jax.numpy as jnp
from jax import lax
from jax.experimental import pallas as pl
from jax.experimental.pallas import tpu as pltpu
from jax.sharding import PartitionSpec as P

FAN1 = 25
FAN2 = 10
LANES = 128
WORDS = 32
EARLY = 1
MIB = 1 << 20

VMEM = pl.BlockSpec(memory_space=pltpu.VMEM)
HBM = pl.BlockSpec(memory_space=pltpu.HBM)
SMEM = pl.BlockSpec(memory_space=pltpu.SMEM)


def in_hbm(value):
    return pltpu.with_memory_space_constraint(value, pltpu.HBM)


def from_ahead(value, axis, steps):
    count = lax.axis_size(axis)
    pairs = [(source, (source - steps) % count) for source in range(count)]
    return lax.ppermute(value, axis, pairs)


def pack_kernel(*refs):
    sources, out_ref, held, (scr, cat, sems) = refs[:5], refs[5], refs[6:11], refs[11:]
    copies = [
        pltpu.make_async_copy(source, place, sems.at[index])
        for index, (source, place) in enumerate(zip(sources, held))
    ]
    for copy in copies:
        copy.start()
    x_ref, ws_ref, wn_ref, us_ref, un_ref = held
    rows, cols = x_ref.shape
    hid = ws_ref.shape[1]
    classes, depth = us_ref.shape
    height = out_ref.shape[0]
    side = cols + 2 * hid
    scr[rows:, :] = jnp.zeros((height - rows, side), jnp.float32)
    cat[...] = jnp.zeros_like(cat)
    for copy in copies:
        copy.wait()
    scr[:rows, :cols] = x_ref[...].astype(jnp.float32)
    scr[:rows, cols : cols + hid] = ws_ref[...].astype(jnp.float32)
    scr[:rows, cols + hid :] = wn_ref[...].astype(jnp.float32)
    cat[:classes, :depth] = us_ref[...].astype(jnp.float32)
    cat[LANES // 2 : LANES // 2 + classes, :depth] = un_ref[...].astype(jnp.float32)
    by_unit = cat[...].T
    out_ref[:, :side] = scr[...].astype(jnp.bfloat16)
    for piece in range(depth // height):
        place = slice(side + piece * LANES, side + (piece + 1) * LANES)
        out_ref[:, place] = by_unit[piece * height : (piece + 1) * height].astype(jnp.bfloat16)


def packed_bits(piece, first_bit):
    words = None
    for group in range(piece.shape[0] // WORDS):
        bits = piece[group * WORDS : (group + 1) * WORDS, :] << (first_bit + group)
        words = bits if words is None else words | bits
    return words


def pack_slot(pieces, first_bit):
    words = None
    for index, arrived in enumerate(pieces):
        piece = arrived()
        bits = packed_bits(piece, first_bit + index * (piece.shape[0] // WORDS))
        words = bits if words is None else words | bits
    return words


def load_kernel(
    nodes, e1_ref, e2_ref, need_ref, live_ref, after_ref, e1_out, bits_ref, number_ref, need, live, number, held, sems
):
    rows = held.shape[1]
    cols = e1_out.shape[0]
    per_slot = cols // rows
    extra = held.shape[0] - 2 * per_slot
    sources = [e1_ref.at[pl.ds(index * rows, rows)] for index in range(per_slot)]
    sources += [e2_ref.at[pl.ds(cols + index * rows, rows)] for index in range(per_slot)]
    sources += [e2_ref.at[pl.ds(3 * cols + index * rows, rows)] for index in range(extra)]
    copies = [
        pltpu.make_async_copy(source, held.at[index], sems.at[index])
        for index, source in enumerate(sources)
    ]
    small = [
        pltpu.make_async_copy(need_ref, need, sems.at[len(sources)]),
        pltpu.make_async_copy(live_ref, live, sems.at[len(sources) + 1]),
    ]
    for copy in small + copies:
        copy.start()
    for copy in small:
        copy.wait()
    offset = lax.rem(need[0, 3] - lax.axis_index("node") + nodes, nodes)
    number[0] = offset - 1 - (offset > nodes // 2).astype(jnp.int32)
    told = pltpu.make_async_copy(number, number_ref, sems.at[len(sources) + 2])
    told.start()

    def arrived(index):
        copies[index].wait()
        return held.at[index]

    for index in range(per_slot):
        piece = arrived(index)[...].astype(jnp.float32).astype(jnp.bfloat16)
        e1_out[index * rows : (index + 1) * rows, :] = piece
    for place, slot, begin, count in ((0, 1, per_slot, per_slot), (1, 3, 2 * per_slot, extra)):
        pieces = [functools.partial(arrived, begin + index) for index in range(count)]
        bits_ref[place] = jnp.where(live[0, slot] == 1, pack_slot(pieces, 0), 0)
    told.wait()


def stream_kernel(z_ref, self_ref, e2_ref, live_ref, total_ref, bits_ref, held, acc, live, sems):
    rows = held.shape[1]
    cols = z_ref.shape[1]
    pieces = cols // rows
    late = held.shape[0] - 2 * pieces
    sources = [slot * pieces + index for slot in (0, 2) for index in range(pieces)]
    sources += [4 * pieces - late + index for index in range(late)]
    copies = [
        pltpu.make_async_copy(e2_ref.at[pl.ds(source * rows, rows)], held.at[index], sems.at[index])
        for index, source in enumerate(sources)
    ]
    copies.append(pltpu.make_async_copy(live_ref, live, sems.at[len(sources)]))
    for copy in copies:
        copy.start()
    acc[...] = jnp.zeros_like(acc)

    def arrived(index):
        pltpu.make_async_copy(e2_ref.at[pl.ds(0, rows)], held.at[index], sems.at[index]).wait()
        return held.at[index]

    @pl.loop(0, pieces)
    def _(index):
        adjacency = arrived(index)[...].astype(jnp.float32).astype(jnp.bfloat16)
        own = z_ref[:, pl.ds(pl.multiple_of(index * rows, rows), rows)]
        acc[...] += jnp.dot(own, adjacency, preferred_element_type=jnp.float32)

    total_ref[...] = self_ref[...] + acc[...] / FAN2
    bits_ref[...] = jnp.zeros_like(bits_ref)

    for place, begin, count in ((0, pieces, pieces), (1, 2 * pieces, late)):

        @pl.loop(0, count)
        def _(index):
            first_bit = (index + pieces - count) * (rows // WORDS)
            bits_ref[place] = bits_ref[place] | packed_bits(arrived(begin + index), first_bit)

    copies[-1].wait()
    for place, slot in enumerate((2, 3)):
        bits_ref[place] = jnp.where(live[0, slot] == 1, bits_ref[place], 0)


def first_kernel(
    hid, depth, p0_ref, p2_ref, p1_ref, p3_ref, e_ref, after_ref, self_ref, z_ref, send_ref, own_ref, x, w1, w2
):
    me = lax.axis_index("feat")
    height = p0_ref.shape[0]
    cols = x.shape[1]
    feats = x.shape[0] // height
    padded = z_ref.shape[0]
    for step, ref in enumerate((p0_ref, p1_ref, p2_ref, p3_ref)):
        place = lax.rem(me + step, feats)
        rows = pl.ds(pl.multiple_of(place * height, height), height)
        x[rows, :] = ref[:, :cols]
        w1[rows, :] = ref[:, cols : cols + hid]
        below = pl.ds(pl.multiple_of((feats + place) * height, height), height)
        w1[below, :] = ref[:, cols + hid : cols + 2 * hid]
        for piece in range(depth // height):
            units = pl.ds(pl.multiple_of(place * depth + piece * height, height), height)
            lanes = slice(cols + 2 * hid + piece * LANES, cols + 2 * hid + (piece + 1) * LANES)
            w2[units, :] = ref[:, lanes]
    inputs = x[...]
    weights = w1[...].astype(jnp.float32).T.astype(jnp.bfloat16)
    project = w2[...].astype(jnp.float32).T.astype(jnp.bfloat16)
    group = lax.broadcasted_iota(jnp.int32, (1, cols), 1) // WORDS
    scale = jnp.ones((1, cols), jnp.float32)
    for bit in range(5):
        scale = scale * jnp.where((group >> bit) % 2 == 1, 2.0 ** -(1 << bit), 1.0)
    scale = jnp.where(group == 31, -scale, scale)
    nbr = jnp.dot(inputs, e_ref[...], preferred_element_type=jnp.float32) / FAN1
    stacked = jnp.concatenate([inputs, nbr.astype(jnp.bfloat16)], axis=0)
    before = jnp.dot(weights, stacked, preferred_element_type=jnp.float32)
    hidden = jnp.maximum(before, 0.0).astype(jnp.bfloat16)
    both = jnp.dot(project, hidden, preferred_element_type=jnp.float32)
    self_ref[...] = both[:padded]
    z = both[LANES // 2 : LANES // 2 + padded]
    own_ref[...] = z.astype(jnp.bfloat16)
    scaled = (z * scale).astype(jnp.bfloat16)
    z_ref[...] = scaled
    send_ref[...] = scaled


def second_kernel(
    classes, z2_ref, z1_ref, z3_ref, total_ref, b13_ref, b23_ref, label_ref, loss_ref, sum_ref, acc
):
    padded, cols = total_ref.shape
    chunk = 256

    def edges(words):
        planes = []
        for bit in range(32):
            mask = (1 << bit) if bit < 31 else -(1 << 31)
            planes.append((words & jnp.int32(mask)).astype(jnp.float32).astype(jnp.bfloat16))
        return jnp.concatenate(planes, axis=0)

    for first in range(0, cols, chunk):
        part = slice(first, first + chunk)
        term = jnp.dot(z1_ref[...], edges(b13_ref[0, :, part]), preferred_element_type=jnp.float32)
        acc[:, part] = term + jnp.dot(
            z2_ref[...], edges(b23_ref[0, :, part]), preferred_element_type=jnp.float32
        )
    class_ids = lax.broadcasted_iota(jnp.int32, (padded, chunk), 0)
    summed = jnp.zeros((1, chunk), jnp.float32)
    for first in range(0, cols, chunk):
        part = slice(first, first + chunk)
        term = acc[:, part] + jnp.dot(
            z3_ref[...],
            edges(b13_ref[1, :, part] | b23_ref[1, :, part]), preferred_element_type=jnp.float32
        )
        logits = total_ref[:, part] + term / FAN2
        powers = jnp.where(class_ids < classes, jnp.exp(logits), 0.0)
        picked = jnp.where(class_ids == label_ref[:, part], logits, 0.0)
        loss = jnp.log(jnp.sum(powers, 0, keepdims=True)) - jnp.sum(picked, 0, keepdims=True)
        loss_ref[:, part] = loss
        summed = summed + loss
    mean = jnp.sum(summed, keepdims=True) / (cols * sum_ref.shape[0])
    sum_ref[...] = jnp.broadcast_to(mean.reshape(1, 1, 1), sum_ref.shape)


def hand_on_kernel(in_ref, out_ref):
    out_ref[...] = in_ref[...]


def final_kernel(loss_ref, parts_ref, out_ref, mean_ref):
    out_ref[...] = loss_ref[...]
    mean_ref[0, 0] = jnp.sum(parts_ref[:, :, 0:1])


def local(
    features,
    edges_one,
    w1_self,
    w1_nbr,
    need_blocks,
    live_slots,
    edges_two,
    w2_self,
    w2_nbr,
    labels,
):
    rows, block_len = features.shape
    hid = w1_self.shape[1]
    depth, classes = w2_self.shape
    nodes = lax.axis_size("node")
    feats = lax.axis_size("feat")
    height = pl.cdiv(rows, 8) * 8
    width = block_len + 2 * hid + depth // height * LANES
    padded = pl.cdiv(classes, 16) * 16

    packed = pl.pallas_call(
        pack_kernel,
        out_shape=jax.ShapeDtypeStruct((height, width), jnp.bfloat16),
        in_specs=[HBM] * 5,
        out_specs=VMEM,
        scratch_shapes=[
            pltpu.VMEM((rows, block_len), jnp.bfloat16),
            pltpu.VMEM((rows, hid), jnp.bfloat16),
            pltpu.VMEM((rows, hid), jnp.bfloat16),
            pltpu.VMEM((classes, depth), jnp.bfloat16),
            pltpu.VMEM((classes, depth), jnp.bfloat16),
            pltpu.VMEM((height, block_len + 2 * hid), jnp.float32),
            pltpu.VMEM((LANES, LANES), jnp.float32),
            pltpu.SemaphoreType.DMA((5,)),
        ],
        compiler_params=pltpu.CompilerParams(vmem_limit_bytes=4 * MIB),
        cost_estimate=pl.CostEstimate(flops=2 * MIB, bytes_accessed=MIB // 4, transcendentals=0),
        name="pack",
    )(*map(in_hbm, (features, w1_self, w1_nbr, w2_self.T, w2_nbr.T)))

    blocks = [packed] + [from_ahead(packed, "feat", step) for step in (2, 1, 3)]
    words = block_len // 32
    adjacency, bits_outer, number = pl.pallas_call(
        functools.partial(load_kernel, nodes),
        out_shape=(
            jax.ShapeDtypeStruct(edges_one.shape, jnp.bfloat16),
            jax.ShapeDtypeStruct((2, words, block_len), jnp.int32),
            jax.ShapeDtypeStruct((1,), jnp.int32),
        ),
        in_specs=[HBM] * 4 + [VMEM],
        out_specs=(VMEM, VMEM, HBM),
        scratch_shapes=[
            pltpu.SMEM(need_blocks.shape, jnp.int32),
            pltpu.SMEM(live_slots.shape, jnp.int32),
            pltpu.SMEM((1,), jnp.int32),
            pltpu.VMEM((8 + EARLY, block_len // 4, block_len), jnp.int32),
            pltpu.SemaphoreType.DMA((11 + EARLY,)),
        ],
        compiler_params=pltpu.CompilerParams(vmem_limit_bytes=16 * MIB),
        cost_estimate=pl.CostEstimate(flops=100 * MIB, bytes_accessed=10 * MIB, transcendentals=0),
        name="load",
    )(*map(in_hbm, (edges_one, edges_two, need_blocks, live_slots)), packed)
    taken = (0, nodes // 2, nodes - 1)
    steps = [step for step in range(nodes) if step not in taken]
    number = lax.clamp(0, number[0], len(steps) - 1)

    self_term, mine, send, own = pl.pallas_call(
        functools.partial(first_kernel, hid, depth),
        out_shape=(
            jax.ShapeDtypeStruct((padded, block_len), jnp.float32),
            jax.ShapeDtypeStruct((padded, block_len), jnp.bfloat16),
            jax.ShapeDtypeStruct((padded, block_len), jnp.bfloat16),
            jax.ShapeDtypeStruct((padded, block_len), jnp.bfloat16),
        ),
        in_specs=[VMEM] * 5 + [HBM],
        out_specs=(VMEM,) * 4,
        scratch_shapes=[
            pltpu.VMEM((feats * height, block_len), jnp.bfloat16),
            pltpu.VMEM((2 * feats * height, hid), jnp.bfloat16),
            pltpu.VMEM((feats * depth, LANES), jnp.bfloat16),
        ],
        compiler_params=pltpu.CompilerParams(vmem_limit_bytes=16 * MIB),
        cost_estimate=pl.CostEstimate(
            flops=2 * 128 * block_len * block_len, bytes_accessed=4 * MIB, transcendentals=0
        ),
        name="first",
    )(*blocks, adjacency, in_hbm(number[None]))

    behind = from_ahead(mine, "node", nodes - 1)
    half = from_ahead(mine, "node", nodes // 2)

    def with_offset(step, send, own, self_term, edges_two, live_slots):
        fourth = from_ahead(send, "node", step)
        total, bits_two = pl.pallas_call(
            stream_kernel,
            out_shape=(
                jax.ShapeDtypeStruct((padded, block_len), jnp.float32),
                jax.ShapeDtypeStruct((2, words, block_len), jnp.int32),
            ),
            in_specs=[VMEM, VMEM, HBM, HBM],
            out_specs=(VMEM, VMEM),
            scratch_shapes=[
                pltpu.VMEM((12 - EARLY, block_len // 4, block_len), jnp.int32),
                pltpu.VMEM((padded, block_len), jnp.float32),
                pltpu.SMEM(live_slots.shape, jnp.int32),
                pltpu.SemaphoreType.DMA((13 - EARLY,)),
            ],
            compiler_params=pltpu.CompilerParams(vmem_limit_bytes=16 * MIB),
            cost_estimate=pl.CostEstimate(
                flops=100 * MIB, bytes_accessed=8 * MIB, transcendentals=0
            ),
            name="stream",
        )(own, self_term, in_hbm(edges_two), in_hbm(live_slots))
        fourth = pl.pallas_call(
            hand_on_kernel,
            out_shape=jax.ShapeDtypeStruct(fourth.shape, fourth.dtype),
            in_specs=[VMEM],
            out_specs=VMEM,
            compiler_params=pltpu.CompilerParams(vmem_limit_bytes=1 * MIB),
            name="hand_on",
        )(fourth)
        return fourth, total, bits_two

    fourth, total, bits_two = lax.switch(
        number,
        [functools.partial(with_offset, step) for step in steps],
        send,
        own,
        self_term,
        edges_two,
        live_slots,
    )

    loss, sums = pl.pallas_call(
        functools.partial(second_kernel, classes),
        out_shape=(
            jax.ShapeDtypeStruct((1, block_len), jnp.float32),
            jax.ShapeDtypeStruct((nodes, 1, LANES), jnp.float32),
        ),
        in_specs=[VMEM] * 7,
        out_specs=(VMEM, VMEM),
        scratch_shapes=[pltpu.VMEM((padded, block_len), jnp.float32)],
        compiler_params=pltpu.CompilerParams(vmem_limit_bytes=16 * MIB),
        cost_estimate=pl.CostEstimate(
            flops=2 * 64 * 3 * block_len * block_len,
            bytes_accessed=2 * MIB,
            transcendentals=padded * block_len,
        ),
        name="second",
    )(behind, half, fourth, total, bits_outer, bits_two, labels[None, :])

    everyone = lax.all_to_all(sums, "node", 0, 0, tiled=True)
    node_loss, mean_loss = pl.pallas_call(
        final_kernel,
        out_shape=(
            jax.ShapeDtypeStruct((1, block_len), jnp.float32),
            jax.ShapeDtypeStruct((1, 1), jnp.float32),
        ),
        in_specs=[VMEM, VMEM],
        out_specs=(VMEM, SMEM),
        compiler_params=pltpu.CompilerParams(vmem_limit_bytes=1 * MIB),
        name="final",
    )(loss, everyone)
    return (node_loss[0], mean_loss[0, 0])


def solution(mesh):
    return jax.shard_map(
        local,
        mesh=mesh,
        in_specs=(
            P("feat", "node"),
            P(None, "node"),
            P("feat", None),
            P("feat", None),
            P("node", None),
            P("node", None),
            P(None, "node"),
            P("feat", None),
            P("feat", None),
            P("node"),
        ),
        out_specs=(P("node"), P()),
        check_vma=False,
    )
```
